32 devices in a mesh: orb: 4 (over x, core), gx: 2 (over y), gyz: 4 (over z).
Axes of the slice: x: 2, y: 2, z: 4, core: 2. Of those that a mesh axis runs over, the one named last changes fastest.
Arguments:
- orbitals: float32 [2, 12, 32, 32, 128], P(None, 'orb', 'gx', 'gyz'), parts along dimension 1, may hold values from -12 to 12
- potential: float32 [32, 32, 128], P('gx', 'gyz'), may hold values from -8 to 60
Outputs:
- evolved: float32 [2, 12, 32, 32, 128], P(None, 'orb', 'gx', 'gyz'), parts along dimension 1
- residual: float32 [2, 12, 32, 32, 128], P(None, 'orb', 'gx', 'gyz'), parts along dimension 1
The draws below stay inside these ranges and needn't reach their ends.
There are 4 independent parts, one for each index of `orb`. The reference program is written for one: setup_inputs(seed, part) draws one part's arguments, and reference() takes and returns one part's arrays. A program takes and returns all parts, laid end to end along the dimension named above; an argument that names none is the same for every part. Nothing has to cross between parts.
All inputs are finite; a program needn't handle non-finite values.
Results may differ from the reference program's by a relative error of at most 0.0003.
Values sent between devices are 32-bit elements; how exact they have to be, the bound alone decides.
A program may use at most 64 MiB of HBM per device.

```python
import jax
import jax.numpy as jnp

ORB = 3
NZ = 128
ITERS = 4
NX = 32
NY = 32


def draw_orbitals(key, part):
    shape = (2, ORB, NX, NY, NZ)
    ramp = 1.0 + 2.0 * jnp.arange(NX, dtype=jnp.float32) / (NX - 1)
    envelope = ramp[None, None, :, None, None]
    values = jax.random.normal(jax.random.fold_in(key, 13), shape, jnp.float32)
    return jnp.clip(values, -4.0, 4.0) * envelope


def draw_potential(key, part):
    rough = jax.random.uniform(jax.random.fold_in(key, 21), (NX, NY, NZ), jnp.float32, -8.0, 8.0)
    ramp = 40.0 * jnp.arange(NX, dtype=jnp.float32)[:, None, None] / (NX - 1)
    return rough + ramp


def setup_inputs(seed: int = 0, part: int = 0) -> dict:
    splits = jax.random.split(jax.random.key(seed), 3)
    own_keys = jax.random.split(jax.random.fold_in(splits[2], part), 3)
    return {
        "orbitals": draw_orbitals(jax.random.fold_in(jax.random.fold_in(splits[2], part), 71), part),
        "potential": draw_potential(jax.random.fold_in(splits[2], 71), part),
    }


SPACING = 0.25
HALF_STEP = 0.05
COEFF_NEAR = 4.0 / 3.0
COEFF_FAR = -1.0 / 12.0
COEFF_SELF = -2.5


def laplace_apply(padded, potential):
    extent = (padded.shape[2] - 4, padded.shape[3] - 4, padded.shape[4] - 4)

    def window(shift_x, shift_y, shift_z):
        return padded[:, :, 2 + shift_x:2 + shift_x + extent[0], 2 + shift_y:2 + shift_y + extent[1], 2 + shift_z:2 + shift_z + extent[2]]

    center = window(0, 0, 0)
    summed = (3.0 * COEFF_SELF) * center
    for offset, weight in ((1, COEFF_NEAR), (2, COEFF_FAR)):
        summed = summed + weight * (window(offset, 0, 0) + window(-offset, 0, 0) + window(0, offset, 0) + window(0, -offset, 0) + window(0, 0, offset) + window(0, 0, -offset))
    return (-0.5 / SPACING ** 2) * summed + potential * center


def hamiltonian(vector, potential):
    padded = jnp.pad(vector, ((0, 0), (0, 0), (2, 2), (2, 2), (2, 2)))
    return laplace_apply(padded, potential)


def system(vector, applied):
    return jnp.stack([vector[0] - HALF_STEP * applied[1], vector[1] + HALF_STEP * applied[0]])


def precondition(vector, potential):
    diagonal = HALF_STEP * (3.75 / SPACING ** 2 + potential)
    divisor = 1.0 + diagonal * diagonal
    return jnp.stack([(vector[0] + diagonal * vector[1]) / divisor, (vector[1] - diagonal * vector[0]) / divisor])


def braket(left, right):
    real_part = jnp.sum(left[0] * right[0] + left[1] * right[1], axis=(1, 2, 3))
    imag_part = jnp.sum(left[0] * right[1] - left[1] * right[0], axis=(1, 2, 3))
    return real_part, imag_part


def times_complex(first, second):
    return (first[0] * second[0] - first[1] * second[1], first[0] * second[1] + first[1] * second[0])


def divide_complex(first, second):
    modulus = second[0] * second[0] + second[1] * second[1]
    return ((first[0] * second[0] + first[1] * second[1]) / modulus, (first[1] * second[0] - first[0] * second[1]) / modulus)


def scale_complex(coeff, vector):
    real_coef = coeff[0][:, None, None, None]
    imag_coef = coeff[1][:, None, None, None]
    return jnp.stack([real_coef * vector[0] - imag_coef * vector[1], real_coef * vector[1] + imag_coef * vector[0]])


def reference(orbitals, potential):
    h_orbitals = hamiltonian(orbitals, potential)
    residual = jnp.stack([2.0 * HALF_STEP * h_orbitals[1], -2.0 * HALF_STEP * h_orbitals[0]])
    evolved = orbitals
    shadow = residual
    direction = residual
    rho_now = braket(shadow, residual)
    for iteration in range(ITERS):
        dir_hat = precondition(direction, potential)
        image = system(dir_hat, hamiltonian(dir_hat, potential))
        alpha_step = divide_complex(rho_now, braket(shadow, image))
        half_step = residual - scale_complex(alpha_step, image)
        half_hat = precondition(half_step, potential)
        second = system(half_hat, hamiltonian(half_hat, potential))
        cross = braket(second, half_step)
        norm_second = jnp.sum(second * second, axis=(0, 2, 3, 4))
        omega_step = (cross[0] / norm_second, cross[1] / norm_second)
        evolved = evolved + scale_complex(alpha_step, dir_hat) + scale_complex(omega_step, half_hat)
        residual = half_step - scale_complex(omega_step, second)
        if iteration + 1 < ITERS:
            rho_next = braket(shadow, residual)
            beta_step = times_complex(divide_complex(rho_next, rho_now), divide_complex(alpha_step, omega_step))
            direction = residual + scale_complex(beta_step, direction - scale_complex(omega_step, image))
            rho_now = rho_next
    return evolved, residual
```

```python
import functools

import jax
import jax.numpy as jnp
from jax import lax
from jax.experimental import pallas as pl
from jax.experimental.pallas import tpu as pltpu
from jax.sharding import PartitionSpec as P

ITERS = 4


SPACING = 0.25
HALF_STEP = 0.05
COEFF_NEAR = 4.0 / 3.0
COEFF_FAR = -1.0 / 12.0
COEFF_SELF = -2.5


def with_halo(array, sides, width):
    for axis, dim in sides:
        size, length = (lax.axis_size(axis), array.shape[dim])
        up = [(i, (i + 1) % size) for i in range(size - 1)]
        down = [(j, i) for i, j in up]
        last = lax.slice_in_dim(array, length - width, length, axis=dim)
        leading = lax.slice_in_dim(array, 0, width, axis=dim)
        before = lax.ppermute(last, axis, up)
        after = lax.ppermute(leading, axis, down)
        array = jnp.concatenate([before, array, after], axis=dim)
    return array


def laplace_apply(padded, potential):
    extent = (padded.shape[2] - 4, padded.shape[3] - 4, padded.shape[4] - 4)

    def window(shift_x, shift_y, shift_z):
        return padded[
            :,
            :,
            2 + shift_x : 2 + shift_x + extent[0],
            2 + shift_y : 2 + shift_y + extent[1],
            2 + shift_z : 2 + shift_z + extent[2],
        ]

    center = window(0, 0, 0)
    summed = 3.0 * COEFF_SELF * center
    for offset, weight in ((1, COEFF_NEAR), (2, COEFF_FAR)):
        summed = summed + weight * (
            window(offset, 0, 0)
            + window(-offset, 0, 0)
            + window(0, offset, 0)
            + window(0, -offset, 0)
            + window(0, 0, offset)
            + window(0, 0, -offset)
        )
    return -0.5 / SPACING**2 * summed + potential * center


def pad_depth(vector):
    return jnp.pad(vector, ((0, 0), (0, 0), (0, 0), (0, 0), (2, 2)))


def system(vector, applied):
    return jnp.stack([vector[0] - HALF_STEP * applied[1], vector[1] + HALF_STEP * applied[0]])


def precondition(vector, potential):
    diagonal = HALF_STEP * (3.75 / SPACING**2 + potential)
    divisor = 1.0 + diagonal * diagonal
    return jnp.stack(
        [(vector[0] + diagonal * vector[1]) / divisor, (vector[1] - diagonal * vector[0]) / divisor]
    )


def braket(left, right):
    real_part = jnp.sum(left[0] * right[0] + left[1] * right[1], axis=(1, 2, 3))
    imag_part = jnp.sum(left[0] * right[1] - left[1] * right[0], axis=(1, 2, 3))
    return (real_part, imag_part)


def times_complex(first, second):
    return (
        first[0] * second[0] - first[1] * second[1],
        first[0] * second[1] + first[1] * second[0],
    )


def divide_complex(first, second):
    modulus = second[0] * second[0] + second[1] * second[1]
    return (
        (first[0] * second[0] + first[1] * second[1]) / modulus,
        (first[1] * second[0] - first[0] * second[1]) / modulus,
    )


def scale_complex(coeff, vector):
    real_coef = coeff[0][:, None, None, None]
    imag_coef = coeff[1][:, None, None, None]
    return jnp.stack(
        [
            real_coef * vector[0] - imag_coef * vector[1],
            real_coef * vector[1] + imag_coef * vector[0],
        ]
    )


def shards(orbitals, potential):

    def apply_shallow(vector):
        padded = with_halo(vector, (("gx", 2), ("gyz", 3)), 2)
        return laplace_apply(pad_depth(padded), potential)

    h_orbitals = apply_shallow(orbitals)
    residual = jnp.stack([2.0 * HALF_STEP * h_orbitals[1], -2.0 * HALF_STEP * h_orbitals[0]])
    evolved = orbitals
    shadow = residual
    direction = residual
    rho_now = lax.psum(braket(shadow, residual), ("gx", "gyz"))
    for iteration in range(ITERS):
        dir_hat = precondition(direction, potential)
        image = system(dir_hat, apply_shallow(dir_hat))
        alpha_step = divide_complex(rho_now, lax.psum(braket(shadow, image), ("gx", "gyz")))
        half_step = residual - scale_complex(alpha_step, image)
        half_hat = precondition(half_step, potential)
        second = system(half_hat, apply_shallow(half_hat))
        cross_local = braket(second, half_step)
        norm_local = jnp.sum(second * second, axis=(0, 2, 3, 4))
        shadow_half = braket(shadow, half_step)
        shadow_second = braket(shadow, second)
        summed = lax.psum(
            (
                cross_local[0],
                cross_local[1],
                norm_local,
                shadow_half[0],
                shadow_half[1],
                shadow_second[0],
                shadow_second[1],
            ),
            ("gx", "gyz"),
        )
        cross_real, cross_imag, norm_second = (summed[0], summed[1], summed[2])
        omega_step = (cross_real / norm_second, cross_imag / norm_second)
        evolved = evolved + scale_complex(alpha_step, dir_hat) + scale_complex(omega_step, half_hat)
        residual = half_step - scale_complex(omega_step, second)
        if iteration + 1 < ITERS:
            along_second = times_complex(omega_step, (summed[5], summed[6]))
            rho_next = (summed[3] - along_second[0], summed[4] - along_second[1])
            beta_step = times_complex(
                divide_complex(rho_next, rho_now), divide_complex(alpha_step, omega_step)
            )
            direction = residual + scale_complex(
                beta_step, direction - scale_complex(omega_step, image)
            )
            rho_now = rho_next
    return (evolved, residual)


UNROLL = 16
LEAD = 8
HALO = 4
POWERS = 2 * ITERS
ROUNDS = ITERS + 1
NEAR = -0.5 / SPACING**2 * COEFF_NEAR * HALF_STEP
FAR = -0.5 / SPACING**2 * COEFF_FAR * HALF_STEP
SIDES = ((0, -1), (0, 1), (-1, -1), (-1, 1), (1, -1), (1, 1), (-1, 0), (1, 0))


def sweep(count, plane, carry):
    width = UNROLL if count % UNROLL == 0 else 1

    def group(i, carry):
        for k in range(width):
            carry = plane(i * width + k, carry)
        return carry

    return lax.fori_loop(0, count // width, group, carry)


def power(vector):
    zero = jnp.zeros_like(vector[0][0])
    padded = vector + [(zero, zero)]
    out = [padded[0]]
    for j in range(1, len(padded)):
        out.append((padded[j][0] + padded[j - 1][0], padded[j][1] + padded[j - 1][1]))
    return out


def add_scaled(base, scale, vector):
    out = []
    for j in range(max(len(base), len(vector))):
        if j >= len(vector):
            out.append(base[j])
            continue
        term = times_complex(scale, vector[j])
        out.append((base[j][0] + term[0], base[j][1] + term[1]) if j < len(base) else term)
    return out


def negated(value):
    return (-value[0], -value[1])


def recurrence(gram):
    def times_gram(i, vector):
        total = None
        for j, value in enumerate(vector):
            term = times_complex(gram(i, j), value)
            total = term if total is None else (total[0] + term[0], total[1] + term[1])
        return total

    def conj_dot(left, right):
        total = None
        for a, b in zip(left, right):
            term = (a[0] * b[0] + a[1] * b[1], a[0] * b[1] - a[1] * b[0])
            total = term if total is None else (total[0] + term[0], total[1] + term[1])
        return total

    one = jnp.ones_like(gram(0, 0)[0])
    unit = [(one, jnp.zeros_like(one))]
    residual, direction, change = unit, unit, []
    rho = times_gram(0, residual)
    for iteration in range(ITERS):
        image = power(direction)
        alpha = divide_complex(rho, times_gram(0, image))
        half = add_scaled(residual, negated(alpha), image)
        second = power(half)
        applied = [times_gram(i, second) for i in range(len(second))]
        cross = conj_dot(half, applied)
        norm = conj_dot(second, applied)[0]
        omega = (cross[0] / norm, -cross[1] / norm)
        change = add_scaled(add_scaled(change, alpha, direction), omega, half)
        residual = add_scaled(half, negated(omega), second)
        if iteration + 1 < ITERS:
            rho_next = times_gram(0, residual)
            beta = times_complex(divide_complex(rho_next, rho), divide_complex(alpha, omega))
            inner = add_scaled(direction, negated(omega), image)
            direction = add_scaled(residual, beta, inner)
            rho = rho_next
    return change, residual


def solve_kernel(
    sizes,
    orb_hbm,
    pot_hbm,
    evolved_ref,
    residual_ref,
    fields,
    inner,
    basis,
    pot,
    diag,
    quot,
    quot_d,
    partial,
    gram_own,
    gram_all,
    send_sem,
    recv_sem,
    send_pot,
    recv_pot,
    send_gram,
    recv_gram,
    local_sem,
):
    size_x, size_y = sizes
    count, bx, by, nz = evolved_ref.shape[1:]
    gx, gy = (lax.axis_index("gx"), lax.axis_index("gyz"))
    me = gx * size_y + gy
    devices = size_x * size_y
    rows = slice(LEAD, LEAD + by)
    planes = slice(HALO, HALO + bx)

    def has(dx, dy):
        x, y = (gx + dx, gy + dy)
        inside = jnp.logical_and(x >= 0, x < size_x)
        return jnp.logical_and(inside, jnp.logical_and(y >= 0, y < size_y))

    def loads(o):
        return pltpu.make_async_copy(
            orb_hbm.at[:, o], fields.at[0, :, o, planes, rows, :], local_sem.at[o]
        )

    load_pot = pltpu.make_async_copy(
        pot_hbm, pot.at[pl.ds(2, bx), pl.ds(LEAD, by), :], local_sem.at[count]
    )
    load_pot.start()
    for o in range(count):
        loads(o).start()

    barrier = pltpu.get_barrier_semaphore()
    partners = 0
    for dx, dy in SIDES:
        there = has(dx, dy)
        partners = partners + there.astype(jnp.int32)

        @pl.when(there)
        def _():
            pl.semaphore_signal(
                barrier,
                inc=1,
                device_id={"gx": gx + dx, "gyz": gy + dy},
                device_id_type=pl.DeviceIdType.MESH,
            )

    def spans(d, first, extent, depth):
        if d == 0:
            return (pl.ds(first, extent), pl.ds(first, extent))
        if d > 0:
            return (pl.ds(first + extent - depth, depth), pl.ds(first - depth, depth))
        return (pl.ds(first, depth), pl.ds(first + extent, depth))

    def remote(src, dst, send, recv, dx, dy):
        return pltpu.make_async_remote_copy(
            src_ref=src,
            dst_ref=dst,
            send_sem=send,
            recv_sem=recv,
            device_id={"gx": gx + dx, "gyz": gy + dy},
            device_id_type=pl.DeviceIdType.MESH,
        )

    def halo_copy(r, o, k):
        dx, dy = SIDES[k]
        depth = 2 if (r == ROUNDS - 1 or (dx and dy)) else HALO
        sx, tx = spans(dx, HALO, bx, depth)
        sy, ty = spans(dy, LEAD, by, depth)
        return remote(
            fields.at[r, :, o, sx, sy, :],
            fields.at[r, :, o, tx, ty, :],
            send_sem.at[r, o, k],
            recv_sem.at[r, o, k],
            dx,
            dy,
        )

    def pot_copy(k):
        dx, dy = SIDES[k]
        sx, tx = spans(dx, 2, bx, 2)
        sy, ty = spans(dy, LEAD, by, 2)
        return remote(
            pot.at[sx, sy, :], pot.at[tx, ty, :], send_pot.at[k], recv_pot.at[k], dx, dy
        )

    def straight(k):
        return SIDES[k][0] == 0 or SIDES[k][1] == 0

    def ways(r):
        return [k for k in range(len(SIDES)) if r < ROUNDS - 1 or straight(k)]

    def send_halo(r, o):
        for k in ways(r):
            @pl.when(has(*SIDES[k]))
            def _():
                halo_copy(r, o, k).start()

    def wait_halo(r, o):
        for k in ways(r):
            @pl.when(has(-SIDES[k][0], -SIDES[k][1]))
            def _():
                halo_copy(r, o, k).wait_recv()

    def clear_edges(ref, halo):
        width, height = ref.shape[-3:-1]
        lead = ref.shape[:-3]
        flat = [()]
        for extent in lead:
            flat = [index + (i,) for index in flat for i in range(extent)]
        low, high = (LEAD - HALO, LEAD + by)

        def side(edge, first, stop):
            @pl.when(edge)
            def _():
                def clear(x, carry):
                    for index in flat:
                        ref[index + (x,)] = jnp.zeros((height, nz), jnp.float32)
                    return carry

                lax.fori_loop(first, stop, clear, 0)

        def band(edge, start):
            @pl.when(edge)
            def _():
                def clear(x, carry):
                    for index in flat:
                        ref[index + (x, slice(start, start + HALO))] = jnp.zeros(
                            (HALO, nz), jnp.float32
                        )
                    return carry

                lax.fori_loop(0, width, clear, 0)

        side(gx == 0, 0, halo)
        side(gx == size_x - 1, width - halo, width)
        band(gy == 0, low)
        band(gy == size_y - 1, high)

    for r in range(ROUNDS):
        clear_edges(fields.at[r], HALO)
    clear_edges(pot, 2)

    pl.semaphore_wait(barrier, partners)
    load_pot.wait()
    for k in range(len(SIDES)):
        if straight(k):
            @pl.when(has(*SIDES[k]))
            def _():
                pot_copy(k).start()
    for o in range(count):
        loads(o).wait()
        send_halo(0, o)

    for k in range(len(SIDES)):
        if straight(k):
            @pl.when(has(-SIDES[k][0], -SIDES[k][1]))
            def _():
                pot_copy(k).wait_recv()

    starts = list(range(-2, by - 5, 8))
    if starts[-1] != by - 6:
        starts.append(by - 6)

    def prepare(x, carry):
        for start in starts:
            span = slice(LEAD + start, LEAD + start + 8)
            d = HALF_STEP * (-1.5 * COEFF_SELF / SPACING**2 + pot[x, span, :])
            q = NEAR / (1.0 + d * d)
            diag[x, span, :] = d
            quot[x, span, :] = q
            quot_d[x, span, :] = q * d
        return carry

    lax.fori_loop(0, bx + 4, prepare, 0)
    for ref in (quot, quot_d):
        clear_edges(ref, 2)

    lane = lax.broadcasted_iota(jnp.int32, (8, nz), 1)

    def offdiagonal(ref, x, y):
        def at(dx, dy):
            return ref[x + dx, y + dy : y + dy + 8, :]

        center = at(0, 0)
        near = (at(1, 0) + at(-1, 0)) + (at(0, 1) + at(0, -1))
        far = (at(2, 0) + at(-2, 0)) + (at(0, 2) + at(0, -2))
        near = near + (
            jnp.where(lane < 1, 0.0, pltpu.roll(center, 1, 1))
            + jnp.where(lane >= nz - 1, 0.0, pltpu.roll(center, nz - 1, 1))
        )
        far = far + (
            jnp.where(lane < 2, 0.0, pltpu.roll(center, 2, 1))
            + jnp.where(lane >= nz - 2, 0.0, pltpu.roll(center, nz - 2, 1))
        )
        return near + (FAR / NEAR) * far, center

    def started(r, o, x, y):
        off_re, re = offdiagonal(fields.at[r, 0, o], x + HALO, LEAD + y)
        off_im, im = offdiagonal(fields.at[r, 1, o], x + HALO, LEAD + y)
        d = diag[x + 2, LEAD + y : LEAD + y + 8, :]
        return 2.0 * (NEAR * off_im + d * im), -2.0 * (NEAR * off_re + d * re)

    def outer(r, o, x, y):
        off_re, _ = offdiagonal(fields.at[r, 0, o], x + HALO, LEAD + y)
        off_im, _ = offdiagonal(fields.at[r, 1, o], x + HALO, LEAD + y)
        return -off_im, off_re

    def hats(x, y, re, im):
        span = slice(LEAD + y, LEAD + y + 8)
        q, qd = (quot[x + 2, span, :], quot_d[x + 2, span, :])
        return q * re + qd * im, q * im - qd * re

    def first_stage(r, o):
        apply = started if r == 0 else outer

        def plane(x, carry):
            for y in starts:
                span = slice(LEAD + y, LEAD + y + 8)
                re, im = apply(r, o, x, y)
                basis[2 * r, 0, o, x, span, :] = re
                basis[2 * r, 1, o, x, span, :] = im
                hat_re, hat_im = hats(x, y, re, im)
                inner[0, x + 2, span, :] = hat_re
                inner[1, x + 2, span, :] = hat_im
            return carry

        for x in (-2, -1, bx, bx + 1):
            for y in range(0, by, 8):
                span = slice(LEAD + y, LEAD + y + 8)
                re, im = apply(r, o, x, y)
                hat_re, hat_im = hats(x, y, re, im)
                inner[0, x + 2, span, :] = hat_re
                inner[1, x + 2, span, :] = hat_im
        sweep(bx, plane, 0)

    def second_stage(r, o):
        def plane(x, carry):
            for y in range(0, by, 8):
                span = slice(LEAD + y, LEAD + y + 8)
                off_re, _ = offdiagonal(inner.at[0], x + 2, LEAD + y)
                off_im, _ = offdiagonal(inner.at[1], x + 2, LEAD + y)
                re, im = -off_im, off_re
                basis[2 * r + 1, 0, o, x, span, :] = re
                basis[2 * r + 1, 1, o, x, span, :] = im
                hat_re, hat_im = hats(x, y, re, im)
                fields[r + 1, 0, o, x + HALO, span, :] = hat_re
                fields[r + 1, 1, o, x + HALO, span, :] = hat_im
            return carry

        sweep(bx, plane, 0)

    def last_stage(r, o):
        def plane(x, carry):
            for y in range(0, by, 8):
                span = slice(LEAD + y, LEAD + y + 8)
                re, im = outer(r, o, x, y)
                basis[2 * r, 0, o, x, span, :] = re
                basis[2 * r, 1, o, x, span, :] = im
            return carry

        sweep(bx, plane, 0)

    size = POWERS + 1
    zero = jnp.zeros((8, nz), jnp.float32)

    def products(j, o):
        def plane(x, sums):
            sums = list(sums)
            for y in range(0, by, 8):
                span = slice(LEAD + y, LEAD + y + 8)
                b_re, b_im = (basis[j, 0, o, x, span, :], basis[j, 1, o, x, span, :])
                for i in range(j):
                    a_re, a_im = (basis[i, 0, o, x, span, :], basis[i, 1, o, x, span, :])
                    sums[2 * i] = sums[2 * i] + (a_re * b_re + a_im * b_im)
                    sums[2 * i + 1] = sums[2 * i + 1] + (a_re * b_im - a_im * b_re)
                sums[2 * j] = sums[2 * j] + (b_re * b_re + b_im * b_im)
            return tuple(sums)

        sums = sweep(bx, plane, (zero,) * (2 * j + 1))
        packed = partial[o]
        for i in range(j + 1):
            packed = jnp.where(
                lane == i * size + j, jnp.sum(sums[2 * i], axis=1, keepdims=True), packed
            )
            if i < j:
                packed = jnp.where(
                    lane == j * size + i, jnp.sum(sums[2 * i + 1], axis=1, keepdims=True), packed
                )
        partial[o] = packed

    for o in range(count):
        partial[o] = zero
    for r in range(ROUNDS):
        last = r == ROUNDS - 1

        def advance(o, carry):
            wait_halo(r, o)
            if last:
                last_stage(r, o)
                products(2 * r, o)
            else:
                first_stage(r, o)
                second_stage(r, o)
                send_halo(r + 1, o)
            return carry

        lax.fori_loop(0, count, advance, 0)
        if not last:
            def gather(o, carry):
                products(2 * r, o)
                products(2 * r + 1, o)
                return carry

            lax.fori_loop(0, count, gather, 0)

    row = lax.broadcasted_iota(jnp.int32, (8, nz), 0)
    packed = zero
    for o in range(count):
        packed = jnp.where(row == o, jnp.sum(partial[o], axis=0, keepdims=True), packed)
    gram_own[...] = packed

    def gram_copy(dev, x, y):
        return pltpu.make_async_remote_copy(
            src_ref=gram_own,
            dst_ref=gram_all.at[dev],
            send_sem=send_gram.at[x * size_y + y],
            recv_sem=recv_gram.at[dev],
            device_id={"gx": x, "gyz": y},
            device_id_type=pl.DeviceIdType.MESH,
        )

    for dev in range(devices):
        @pl.when(me != dev)
        def _():
            gram_copy(me, dev // size_y, dev % size_y).start()

    gram_all[pl.ds(me, 1)] = packed[None]
    for dev in range(devices):
        @pl.when(me != dev)
        def _():
            gram_copy(dev, gx, gy).wait_recv()

    summed = gram_all[0]
    for dev in range(1, devices):
        summed = summed + gram_all[dev]

    def spread(index):
        return jnp.broadcast_to(summed[:, index : index + 1], (8, nz))

    values = {}

    def gram(i, j):
        if i > j:
            re, im = gram(j, i)
            return re, -im
        if (i, j) not in values:
            re = spread(i * size + j)
            values[i, j] = (re, spread(j * size + i) if i < j else jnp.zeros_like(re))
        return values[i, j]

    change, left = recurrence(gram)
    change = [(a / NEAR, b / NEAR) for a, b in change]

    for o in range(count):
        def own(value):
            return jnp.broadcast_to(value[o : o + 1], (8, nz))

        moves = [(own(a), own(b)) for a, b in change]
        rests = [(own(a), own(b)) for a, b in left]

        def finish(x, carry):
            for y in range(0, by, 8):
                span = slice(LEAD + y, LEAD + y + 8)
                s_re = s_im = r_re = r_im = None
                for j in range(size):
                    w_re, w_im = (basis[j, 0, o, x, span, :], basis[j, 1, o, x, span, :])
                    c = rests[j]
                    t_re = c[0] * w_re - c[1] * w_im
                    t_im = c[0] * w_im + c[1] * w_re
                    r_re = t_re if r_re is None else r_re + t_re
                    r_im = t_im if r_im is None else r_im + t_im
                    if j < len(moves):
                        c = moves[j]
                        t_re = c[0] * w_re - c[1] * w_im
                        t_im = c[0] * w_im + c[1] * w_re
                        s_re = t_re if s_re is None else s_re + t_re
                        s_im = t_im if s_im is None else s_im + t_im
                hat_re, hat_im = hats(x, y, s_re, s_im)
                out = slice(y, y + 8)
                evolved_ref[0, o, x, out, :] = fields[0, 0, o, x + HALO, span, :] + hat_re
                evolved_ref[1, o, x, out, :] = fields[0, 1, o, x + HALO, span, :] + hat_im
                residual_ref[0, o, x, out, :] = r_re
                residual_ref[1, o, x, out, :] = r_im
            return carry

        sweep(bx, finish, 0)

    for k in range(len(SIDES)):
        @pl.when(has(*SIDES[k]))
        def _():
            if straight(k):
                pot_copy(k).wait_send()
            for r in range(ROUNDS):
                if k in ways(r):
                    for o in range(count):
                        halo_copy(r, o, k).wait_send()

    for dev in range(devices):
        @pl.when(me != dev)
        def _():
            gram_copy(me, dev // size_y, dev % size_y).wait_send()


def powers(sizes, orbitals, potential):
    size_x, size_y = sizes
    _, count, bx, by, nz = orbitals.shape
    tall = by + 2 * LEAD
    devices = size_x * size_y
    dma = pltpu.SemaphoreType.DMA
    shape = jax.ShapeDtypeStruct(orbitals.shape, jnp.float32)

    def vmem(*dims):
        return pltpu.VMEM(dims, jnp.float32)

    return pl.pallas_call(
        functools.partial(solve_kernel, sizes),
        out_shape=(shape, shape),
        in_specs=[pl.BlockSpec(memory_space=pltpu.HBM)] * 2,
        out_specs=(pl.BlockSpec(memory_space=pltpu.VMEM),) * 2,
        scratch_shapes=[
            vmem(ROUNDS, 2, count, bx + 2 * HALO, tall, nz),
            vmem(2, bx + 4, tall, nz),
            vmem(POWERS + 1, 2, count, bx, tall, nz),
            vmem(bx + 4, tall, nz),
            vmem(bx + 4, tall, nz),
            vmem(bx + 4, tall, nz),
            vmem(bx + 4, tall, nz),
            vmem(count, 8, nz),
            vmem(8, nz),
            vmem(devices, 8, nz),
            dma((ROUNDS, count, len(SIDES))),
            dma((ROUNDS, count, len(SIDES))),
            dma((len(SIDES),)),
            dma((len(SIDES),)),
            dma((devices,)),
            dma((devices,)),
            dma((count + 1,)),
        ],
        compiler_params=pltpu.CompilerParams(
            collective_id=0, has_side_effects=True, vmem_limit_bytes=48 * 1024 * 1024
        ),
    )(orbitals, potential)


def step(sizes, orbitals, potential):
    _, count, bx, by, nz = orbitals.shape
    near = max(sizes) <= ROUNDS
    fits = (POWERS + 2 * ROUNDS) * count * (bx + 8) * (by + 16) * nz <= 1 << 23
    packs = count <= 8 and (POWERS + 1) ** 2 <= nz
    if near and fits and packs and by % 8 == 0 and nz == 128 and bx >= 4:
        return powers(sizes, orbitals, potential)
    return shards(orbitals, potential)


def solution(mesh):
    sizes = (mesh.shape["gx"], mesh.shape["gyz"])
    return jax.shard_map(
        functools.partial(step, sizes),
        mesh=mesh,
        in_specs=(P(None, "orb", "gx", "gyz", None), P("gx", "gyz", None)),
        out_specs=(P(None, "orb", "gx", "gyz", None), P(None, "orb", "gx", "gyz", None)),
        check_vma=False,
    )
```

```python
import functools

import jax
import jax.numpy as jnp
from jax import lax
from jax.experimental import pallas as pl
from jax.experimental.pallas import tpu as pltpu
from jax.sharding import PartitionSpec as P

ITERS = 4


SPACING = 0.25
HALF_STEP = 0.05
COEFF_NEAR = 4.0 / 3.0
COEFF_FAR = -1.0 / 12.0
COEFF_SELF = -2.5


def with_halo(array, sides, width):
    for axis, dim in sides:
        size, length = (lax.axis_size(axis), array.shape[dim])
        up = [(i, (i + 1) % size) for i in range(size - 1)]
        down = [(j, i) for i, j in up]
        last = lax.slice_in_dim(array, length - width, length, axis=dim)
        leading = lax.slice_in_dim(array, 0, width, axis=dim)
        before = lax.ppermute(last, axis, up)
        after = lax.ppermute(leading, axis, down)
        array = jnp.concatenate([before, array, after], axis=dim)
    return array


def laplace_apply(padded, potential):
    extent = (padded.shape[2] - 4, padded.shape[3] - 4, padded.shape[4] - 4)

    def window(shift_x, shift_y, shift_z):
        return padded[
            :,
            :,
            2 + shift_x : 2 + shift_x + extent[0],
            2 + shift_y : 2 + shift_y + extent[1],
            2 + shift_z : 2 + shift_z + extent[2],
        ]

    center = window(0, 0, 0)
    summed = 3.0 * COEFF_SELF * center
    for offset, weight in ((1, COEFF_NEAR), (2, COEFF_FAR)):
        summed = summed + weight * (
            window(offset, 0, 0)
            + window(-offset, 0, 0)
            + window(0, offset, 0)
            + window(0, -offset, 0)
            + window(0, 0, offset)
            + window(0, 0, -offset)
        )
    return -0.5 / SPACING**2 * summed + potential * center


def pad_depth(vector):
    return jnp.pad(vector, ((0, 0), (0, 0), (0, 0), (0, 0), (2, 2)))


def system(vector, applied):
    return jnp.stack([vector[0] - HALF_STEP * applied[1], vector[1] + HALF_STEP * applied[0]])


def precondition(vector, potential):
    diagonal = HALF_STEP * (3.75 / SPACING**2 + potential)
    divisor = 1.0 + diagonal * diagonal
    return jnp.stack(
        [(vector[0] + diagonal * vector[1]) / divisor, (vector[1] - diagonal * vector[0]) / divisor]
    )


def braket(left, right):
    real_part = jnp.sum(left[0] * right[0] + left[1] * right[1], axis=(1, 2, 3))
    imag_part = jnp.sum(left[0] * right[1] - left[1] * right[0], axis=(1, 2, 3))
    return (real_part, imag_part)


def times_complex(first, second):
    return (
        first[0] * second[0] - first[1] * second[1],
        first[0] * second[1] + first[1] * second[0],
    )


def divide_complex(first, second):
    modulus = second[0] * second[0] + second[1] * second[1]
    return (
        (first[0] * second[0] + first[1] * second[1]) / modulus,
        (first[1] * second[0] - first[0] * second[1]) / modulus,
    )


def scale_complex(coeff, vector):
    real_coef = coeff[0][:, None, None, None]
    imag_coef = coeff[1][:, None, None, None]
    return jnp.stack(
        [
            real_coef * vector[0] - imag_coef * vector[1],
            real_coef * vector[1] + imag_coef * vector[0],
        ]
    )


def shards(orbitals, potential):

    def apply_shallow(vector):
        padded = with_halo(vector, (("gx", 2), ("gyz", 3)), 2)
        return laplace_apply(pad_depth(padded), potential)

    h_orbitals = apply_shallow(orbitals)
    residual = jnp.stack([2.0 * HALF_STEP * h_orbitals[1], -2.0 * HALF_STEP * h_orbitals[0]])
    evolved = orbitals
    shadow = residual
    direction = residual
    rho_now = lax.psum(braket(shadow, residual), ("gx", "gyz"))
    for iteration in range(ITERS):
        dir_hat = precondition(direction, potential)
        image = system(dir_hat, apply_shallow(dir_hat))
        alpha_step = divide_complex(rho_now, lax.psum(braket(shadow, image), ("gx", "gyz")))
        half_step = residual - scale_complex(alpha_step, image)
        half_hat = precondition(half_step, potential)
        second = system(half_hat, apply_shallow(half_hat))
        cross_local = braket(second, half_step)
        norm_local = jnp.sum(second * second, axis=(0, 2, 3, 4))
        shadow_half = braket(shadow, half_step)
        shadow_second = braket(shadow, second)
        summed = lax.psum(
            (
                cross_local[0],
                cross_local[1],
                norm_local,
                shadow_half[0],
                shadow_half[1],
                shadow_second[0],
                shadow_second[1],
            ),
            ("gx", "gyz"),
        )
        cross_real, cross_imag, norm_second = (summed[0], summed[1], summed[2])
        omega_step = (cross_real / norm_second, cross_imag / norm_second)
        evolved = evolved + scale_complex(alpha_step, dir_hat) + scale_complex(omega_step, half_hat)
        residual = half_step - scale_complex(omega_step, second)
        if iteration + 1 < ITERS:
            along_second = times_complex(omega_step, (summed[5], summed[6]))
            rho_next = (summed[3] - along_second[0], summed[4] - along_second[1])
            beta_step = times_complex(
                divide_complex(rho_next, rho_now), divide_complex(alpha_step, omega_step)
            )
            direction = residual + scale_complex(
                beta_step, direction - scale_complex(omega_step, image)
            )
            rho_now = rho_next
    return (evolved, residual)


UNROLL = 16
LEAD = 8
HALO = 4
VMEM_LIMIT = 48000000
POWERS = 2 * ITERS
ROUNDS = ITERS + 1
NEAR = -0.5 / SPACING**2 * COEFF_NEAR * HALF_STEP
FAR = -0.5 / SPACING**2 * COEFF_FAR * HALF_STEP
SIDES = ((0, -1), (0, 1), (-1, -1), (-1, 1), (1, -1), (1, 1), (-1, 0), (1, 0))


def sweep(count, plane, carry, unroll=UNROLL):
    width = unroll if count % unroll == 0 else 1

    def group(i, carry):
        for k in range(width):
            carry = plane(i * width + k, carry)
        return carry

    return lax.fori_loop(0, count // width, group, carry)


def power(vector):
    zero = jnp.zeros_like(vector[0][0])
    padded = vector + [(zero, zero)]
    out = [padded[0]]
    for j in range(1, len(padded)):
        out.append((padded[j][0] + padded[j - 1][0], padded[j][1] + padded[j - 1][1]))
    return out


def add_scaled(base, scale, vector):
    out = []
    for j in range(max(len(base), len(vector))):
        if j >= len(vector):
            out.append(base[j])
            continue
        term = times_complex(scale, vector[j])
        out.append((base[j][0] + term[0], base[j][1] + term[1]) if j < len(base) else term)
    return out


def negated(value):
    return (-value[0], -value[1])


def plus(first, second):
    if first is None:
        return second
    return (first[0] + second[0], first[1] + second[1])


def conj_times(first, second):
    return (
        first[0] * second[0] + first[1] * second[1],
        first[0] * second[1] - first[1] * second[0],
    )


def conj_dot(left, right):
    total = None
    for a, b in zip(left, right):
        total = plus(total, conj_times(a, b))
    return total


def recurrence(gram):
    def times_gram(i, vector):
        total = None
        for j, value in enumerate(vector):
            total = plus(total, times_complex(gram(i, j), value))
        return total

    one = jnp.ones_like(gram(0, 0)[0])
    unit = [(one, jnp.zeros_like(one))]
    residual, direction, change = unit, unit, []
    rho = times_gram(0, residual)
    for iteration in range(ITERS):
        image = power(direction)
        alpha = divide_complex(rho, times_gram(0, image))
        half = add_scaled(residual, negated(alpha), image)
        second = power(half)
        change = add_scaled(change, alpha, direction)
        if iteration + 1 == ITERS:
            known = [times_gram(i, second[:-1]) for i in range(len(half))]
            cross = conj_dot(half, known)
            norm = conj_dot(second[:-1], known)[0]
            return change, half, second, cross, norm
        applied = [times_gram(i, second) for i in range(len(second))]
        cross = conj_dot(half, applied)
        norm = conj_dot(second, applied)[0]
        omega = (cross[0] / norm, -cross[1] / norm)
        change = add_scaled(change, omega, half)
        residual = add_scaled(half, negated(omega), second)
        rho_next = times_gram(0, residual)
        beta = times_complex(divide_complex(rho_next, rho), divide_complex(alpha, omega))
        inner = add_scaled(direction, negated(omega), image)
        direction = add_scaled(residual, beta, inner)
        rho = rho_next


def closing(column, half, second, cross, norm):
    top = second[-1]
    along = times_complex(top, conj_dot(half, column))
    cross = plus(cross, along)
    across = times_complex(top, conj_dot(second[:-1], column))
    norm = norm + 2.0 * across[0] + (top[0] * top[0] + top[1] * top[1]) * column[-1][0]
    return (cross[0] / norm, -cross[1] / norm)


def solve_kernel(
    sizes,
    orb_hbm,
    pot_hbm,
    evolved_ref,
    residual_ref,
    fields,
    inner,
    basis,
    pot,
    diag,
    quot,
    quot_d,
    second_ref,
    hat_ref,
    partial,
    gram_own,
    gram_all,
    send_sem,
    recv_sem,
    send_pot,
    recv_pot,
    send_gram,
    recv_gram,
    local_sem,
):
    size_x, size_y = sizes
    count, bx, by, nz = evolved_ref.shape[1:]
    gx, gy = (lax.axis_index("gx"), lax.axis_index("gyz"))
    me = gx * size_y + gy
    devices = size_x * size_y
    rows = slice(LEAD, LEAD + by)
    planes = slice(HALO, HALO + bx)

    def has(dx, dy):
        x, y = (gx + dx, gy + dy)
        inside = jnp.logical_and(x >= 0, x < size_x)
        return jnp.logical_and(inside, jnp.logical_and(y >= 0, y < size_y))

    def loads(o):
        return pltpu.make_async_copy(
            orb_hbm.at[:, o], fields.at[0, :, o, planes, rows, :], local_sem.at[o]
        )

    load_pot = pltpu.make_async_copy(
        pot_hbm, pot.at[pl.ds(2, bx), pl.ds(LEAD, by), :], local_sem.at[count]
    )
    load_pot.start()
    for o in range(count):
        loads(o).start()

    barrier = pltpu.get_barrier_semaphore()
    partners = 0
    for dx, dy in SIDES:
        there = has(dx, dy)
        partners = partners + there.astype(jnp.int32)

        @pl.when(there)
        def _():
            pl.semaphore_signal(
                barrier,
                inc=1,
                device_id={"gx": gx + dx, "gyz": gy + dy},
                device_id_type=pl.DeviceIdType.MESH,
            )

    def spans(d, first, extent, depth):
        if d == 0:
            return (pl.ds(first, extent), pl.ds(first, extent))
        if d > 0:
            return (pl.ds(first + extent - depth, depth), pl.ds(first - depth, depth))
        return (pl.ds(first, depth), pl.ds(first + extent, depth))

    def remote(src, dst, send, recv, dx, dy):
        return pltpu.make_async_remote_copy(
            src_ref=src,
            dst_ref=dst,
            send_sem=send,
            recv_sem=recv,
            device_id={"gx": gx + dx, "gyz": gy + dy},
            device_id_type=pl.DeviceIdType.MESH,
        )

    def halo_copy(r, o, k):
        dx, dy = SIDES[k]
        depth = 2 if (r == ROUNDS - 1 or (dx and dy)) else HALO
        sx, tx = spans(dx, HALO, bx, depth)
        sy, ty = spans(dy, LEAD, by, depth)
        return remote(
            fields.at[r, :, o, sx, sy, :],
            fields.at[r, :, o, tx, ty, :],
            send_sem.at[r, o, k],
            recv_sem.at[r, o, k],
            dx,
            dy,
        )

    def pot_copy(k):
        dx, dy = SIDES[k]
        sx, tx = spans(dx, 2, bx, 2)
        sy, ty = spans(dy, LEAD, by, 2)
        return remote(
            pot.at[sx, sy, :], pot.at[tx, ty, :], send_pot.at[k], recv_pot.at[k], dx, dy
        )

    def straight(k):
        return SIDES[k][0] == 0 or SIDES[k][1] == 0

    def ways(r):
        return [k for k in range(len(SIDES)) if r < ROUNDS - 1 or straight(k)]

    def send_halo(r, o):
        for k in ways(r):
            @pl.when(has(*SIDES[k]))
            def _():
                halo_copy(r, o, k).start()

    def wait_halo(r, o):
        for k in ways(r):
            @pl.when(has(-SIDES[k][0], -SIDES[k][1]))
            def _():
                halo_copy(r, o, k).wait_recv()

    def clear_edges(ref, halo):
        width, height = ref.shape[-3:-1]
        lead = ref.shape[:-3]
        flat = [()]
        for extent in lead:
            flat = [index + (i,) for index in flat for i in range(extent)]
        low, high = (LEAD - HALO, LEAD + by)

        def side(edge, first, stop):
            @pl.when(edge)
            def _():
                def clear(x, carry):
                    for index in flat:
                        ref[index + (x,)] = jnp.zeros((height, nz), jnp.float32)
                    return carry

                lax.fori_loop(first, stop, clear, 0)

        def band(edge, start):
            @pl.when(edge)
            def _():
                def clear(x, carry):
                    for index in flat:
                        ref[index + (x, slice(start, start + HALO))] = jnp.zeros(
                            (HALO, nz), jnp.float32
                        )
                    return carry

                lax.fori_loop(0, width, clear, 0)

        side(gx == 0, 0, halo)
        side(gx == size_x - 1, width - halo, width)
        band(gy == 0, low)
        band(gy == size_y - 1, high)

    clear_edges(pot, 2)
    clear_edges(fields.at[0], HALO)

    pl.semaphore_wait(barrier, partners)
    load_pot.wait()
    for k in range(len(SIDES)):
        if straight(k):
            @pl.when(has(*SIDES[k]))
            def _():
                pot_copy(k).start()
    for o in range(count):
        loads(o).wait()
    late = lax.axis_index("orb") % 2 == 1

    def send_first():
        for o in range(count):
            send_halo(0, o)

    pl.when(jnp.logical_not(late))(send_first)

    for r in range(1, ROUNDS):
        clear_edges(fields.at[r], HALO)
    for o in range(count):
        for half in range(2):
            partial[half, o] = jnp.zeros((8, nz), jnp.float32)

    for k in range(len(SIDES)):
        if straight(k):
            @pl.when(has(-SIDES[k][0], -SIDES[k][1]))
            def _():
                pot_copy(k).wait_recv()

    pl.when(late)(send_first)

    starts = list(range(-2, by - 5, 8))
    if starts[-1] != by - 6:
        starts.append(by - 6)

    def prepare(x, carry):
        for start in starts:
            span = slice(LEAD + start, LEAD + start + 8)
            d = HALF_STEP * (-1.5 * COEFF_SELF / SPACING**2 + pot[x, span, :])
            q = NEAR / (1.0 + d * d)
            diag[x, span, :] = d
            quot[x, span, :] = q
            quot_d[x, span, :] = q * d
        return carry

    sweep(bx + 4, prepare, 0, bx + 4)
    for ref in (quot, quot_d):
        clear_edges(ref, 2)

    lane = lax.broadcasted_iota(jnp.int32, (8, nz), 1)

    def offdiagonal(ref, x, y):
        def at(dx, dy):
            return ref[x + dx, y + dy : y + dy + 8, :]

        center = at(0, 0)
        near = (at(1, 0) + at(-1, 0)) + (at(0, 1) + at(0, -1))
        far = (at(2, 0) + at(-2, 0)) + (at(0, 2) + at(0, -2))
        near = near + (
            jnp.where(lane < 1, 0.0, pltpu.roll(center, 1, 1))
            + jnp.where(lane >= nz - 1, 0.0, pltpu.roll(center, nz - 1, 1))
        )
        far = far + (
            jnp.where(lane < 2, 0.0, pltpu.roll(center, 2, 1))
            + jnp.where(lane >= nz - 2, 0.0, pltpu.roll(center, nz - 2, 1))
        )
        return near + (FAR / NEAR) * far, center

    def started(r, o, x, y):
        off_re, re = offdiagonal(fields.at[r, 0, o], x + HALO, LEAD + y)
        off_im, im = offdiagonal(fields.at[r, 1, o], x + HALO, LEAD + y)
        d = diag[x + 2, LEAD + y : LEAD + y + 8, :]
        return 2.0 * (NEAR * off_im + d * im), -2.0 * (NEAR * off_re + d * re)

    def outer(r, o, x, y):
        off_re, _ = offdiagonal(fields.at[r, 0, o], x + HALO, LEAD + y)
        off_im, _ = offdiagonal(fields.at[r, 1, o], x + HALO, LEAD + y)
        return -off_im, off_re

    def hats(x, y, re, im):
        span = slice(LEAD + y, LEAD + y + 8)
        q, qd = (quot[x + 2, span, :], quot_d[x + 2, span, :])
        return q * re + qd * im, q * im - qd * re

    def first_stage(r, o):
        apply = started if r == 0 else outer

        def plane(x, carry):
            for y in starts:
                span = slice(LEAD + y, LEAD + y + 8)
                re, im = apply(r, o, x, y)
                basis[2 * r, 0, o, x, span, :] = re
                basis[2 * r, 1, o, x, span, :] = im
                hat_re, hat_im = hats(x, y, re, im)
                inner[0, x + 2, span, :] = hat_re
                inner[1, x + 2, span, :] = hat_im
            return carry

        for x in (-2, -1, bx, bx + 1):
            for y in range(0, by, 8):
                span = slice(LEAD + y, LEAD + y + 8)
                re, im = apply(r, o, x, y)
                hat_re, hat_im = hats(x, y, re, im)
                inner[0, x + 2, span, :] = hat_re
                inner[1, x + 2, span, :] = hat_im
        sweep(bx, plane, 0)

    def second_stage(r, o):
        def plane(x, carry):
            for y in range(0, by, 8):
                span = slice(LEAD + y, LEAD + y + 8)
                off_re, _ = offdiagonal(inner.at[0], x + 2, LEAD + y)
                off_im, _ = offdiagonal(inner.at[1], x + 2, LEAD + y)
                re, im = -off_im, off_re
                basis[2 * r + 1, 0, o, x, span, :] = re
                basis[2 * r + 1, 1, o, x, span, :] = im
                hat_re, hat_im = hats(x, y, re, im)
                fields[r + 1, 0, o, x + HALO, span, :] = hat_re
                fields[r + 1, 1, o, x + HALO, span, :] = hat_im
            return carry

        sweep(bx, plane, 0)

    def last_stage(r, o):
        def plane(x, carry):
            for y in range(0, by, 8):
                span = slice(LEAD + y, LEAD + y + 8)
                re, im = outer(r, o, x, y)
                basis[2 * r, 0, o, x, span, :] = re
                basis[2 * r, 1, o, x, span, :] = im
            return carry

        sweep(bx, plane, 0)

    size = POWERS + 1
    zero = jnp.zeros((8, nz), jnp.float32)

    def products(j, o):
        def plane(x, sums):
            sums = list(sums)
            for y in range(0, by, 8):
                span = slice(LEAD + y, LEAD + y + 8)
                b_re, b_im = (basis[j, 0, o, x, span, :], basis[j, 1, o, x, span, :])
                for i in range(j):
                    a_re, a_im = (basis[i, 0, o, x, span, :], basis[i, 1, o, x, span, :])
                    sums[2 * i] = sums[2 * i] + (a_re * b_re + a_im * b_im)
                    sums[2 * i + 1] = sums[2 * i + 1] + (a_re * b_im - a_im * b_re)
                sums[2 * j] = sums[2 * j] + (b_re * b_re + b_im * b_im)
            return tuple(sums)

        sums = sweep(bx, plane, (zero,) * (2 * j + 1))
        half = 0 if j < POWERS else 1
        packed = partial[half, o]
        for i in range(j + 1):
            packed = jnp.where(
                lane == i * size + j, jnp.sum(sums[2 * i], axis=1, keepdims=True), packed
            )
            if i < j:
                packed = jnp.where(
                    lane == j * size + i, jnp.sum(sums[2 * i + 1], axis=1, keepdims=True), packed
                )
        partial[half, o] = packed

    row = lax.broadcasted_iota(jnp.int32, (8, nz), 0)

    def gram_copy(half, dev, x, y):
        return pltpu.make_async_remote_copy(
            src_ref=gram_own.at[half],
            dst_ref=gram_all.at[half, dev],
            send_sem=send_gram.at[half, x * size_y + y],
            recv_sem=recv_gram.at[half, dev],
            device_id={"gx": x, "gyz": y},
            device_id_type=pl.DeviceIdType.MESH,
        )

    def share(half):
        packed = zero
        for o in range(count):
            packed = jnp.where(
                row == o, jnp.sum(partial[half, o], axis=0, keepdims=True), packed
            )
        gram_own[half] = packed
        gram_all[half, pl.ds(me, 1)] = packed[None]
        for dev in range(devices):
            @pl.when(me != dev)
            def _():
                gram_copy(half, me, dev // size_y, dev % size_y).start()

    def shared(half):
        for dev in range(devices):
            @pl.when(me != dev)
            def _():
                gram_copy(half, dev, gx, gy).wait_recv()

        summed = gram_all[half, 0]
        for dev in range(1, devices):
            summed = summed + gram_all[half, dev]
        values = {}

        def spread(index):
            return jnp.broadcast_to(summed[:, index : index + 1], (8, nz))

        def gram(i, j):
            if i > j:
                re, im = gram(j, i)
                return re, -im
            if (i, j) not in values:
                re = spread(i * size + j)
                values[i, j] = (re, spread(j * size + i) if i < j else jnp.zeros_like(re))
            return values[i, j]

        return gram

    for r in range(ROUNDS):
        last = r == ROUNDS - 1

        def advance(o, carry):
            wait_halo(r, o)
            if last:
                last_stage(r, o)
                products(2 * r, o)
            else:
                first_stage(r, o)
                second_stage(r, o)
                send_halo(r + 1, o)
            return carry

        lax.fori_loop(0, count, advance, 0)
        if last:
            share(1)
        else:
            def gather(o, carry):
                products(2 * r, o)
                products(2 * r + 1, o)
                return carry

            lax.fori_loop(0, count, gather, 0)
            if r == ROUNDS - 2:
                share(0)

    change, halved, doubled, cross, norm = recurrence(shared(0))
    change = [(a / NEAR, b / NEAR) for a, b in change]

    def combine(o, x, span, coefs):
        total = None
        for j, c in enumerate(coefs):
            term = times_complex(c, (basis[j, 0, o, x, span, :], basis[j, 1, o, x, span, :]))
            total = plus(total, term)
        return total

    for o in range(count):
        def own(values):
            return [
                tuple(jnp.broadcast_to(part[o : o + 1], (8, nz)) for part in value)
                for value in values
            ]

        moves, halves, seconds = (own(change), own(halved), own(doubled))

        def blend(x, carry):
            for y in range(0, by, 8):
                span = slice(LEAD + y, LEAD + y + 8)
                out = slice(y, y + 8)
                for ref, total in (
                    (residual_ref, combine(o, x, span, halves)),
                    (second_ref, combine(o, x, span, seconds)),
                ):
                    ref[0, o, x, out, :] = total[0]
                    ref[1, o, x, out, :] = total[1]
                hat = hats(x, y, residual_ref[0, o, x, out, :], residual_ref[1, o, x, out, :])
                hat_ref[0, o, x, out, :] = hat[0]
                hat_ref[1, o, x, out, :] = hat[1]
                hat = hats(x, y, *combine(o, x, span, moves))
                evolved_ref[0, o, x, out, :] = fields[0, 0, o, x + HALO, span, :] + hat[0]
                evolved_ref[1, o, x, out, :] = fields[0, 1, o, x + HALO, span, :] + hat[1]
            return carry

        sweep(bx, blend, 0)

    for k in range(len(SIDES)):
        @pl.when(has(*SIDES[k]))
        def _():
            if straight(k):
                pot_copy(k).wait_send()
            for r in range(ROUNDS):
                if k in ways(r):
                    for o in range(count):
                        halo_copy(r, o, k).wait_send()

    gram = shared(1)
    column = [gram(i, POWERS) for i in range(size)]
    omega = closing(column, halved, doubled, cross, norm)
    scaled = (omega[0] / NEAR, omega[1] / NEAR)

    for o in range(count):
        step_r, step_e = (
            tuple(jnp.broadcast_to(part[o : o + 1], (8, nz)) for part in value)
            for value in (omega, scaled)
        )

        def finish(x, carry):
            for y in range(0, by, 8):
                out = slice(y, y + 8)
                for ref, other, coef, sign in (
                    (residual_ref, second_ref, step_r, -1.0),
                    (evolved_ref, hat_ref, step_e, 1.0),
                ):
                    term = times_complex(coef, (other[0, o, x, out, :], other[1, o, x, out, :]))
                    ref[0, o, x, out, :] = ref[0, o, x, out, :] + sign * term[0]
                    ref[1, o, x, out, :] = ref[1, o, x, out, :] + sign * term[1]
            return carry

        sweep(bx, finish, 0)

    for half in range(2):
        for dev in range(devices):
            @pl.when(me != dev)
            def _():
                gram_copy(half, me, dev // size_y, dev % size_y).wait_send()


def store_kernel(count, *refs):
    sources, targets, sems = (refs[:count], refs[count : 2 * count], refs[-1])
    copies = [
        pltpu.make_async_copy(sources[k], targets[k], sems.at[k]) for k in range(count)
    ]
    for copy in copies:
        copy.start()
    for copy in copies:
        copy.wait()


def store(arrays):
    count = len(arrays)
    return pl.pallas_call(
        functools.partial(store_kernel, count),
        out_shape=tuple(jax.ShapeDtypeStruct(a.shape, a.dtype) for a in arrays),
        in_specs=[pl.BlockSpec(memory_space=pltpu.VMEM)] * count,
        out_specs=(pl.BlockSpec(memory_space=pltpu.HBM),) * count,
        scratch_shapes=[pltpu.SemaphoreType.DMA((count,))],
        compiler_params=pltpu.CompilerParams(vmem_limit_bytes=1 << 20),
    )(*arrays)


def powers(sizes, orbitals, potential):
    size_x, size_y = sizes
    _, count, bx, by, nz = orbitals.shape
    tall = by + 2 * LEAD
    devices = size_x * size_y
    dma = pltpu.SemaphoreType.DMA
    shape = jax.ShapeDtypeStruct(orbitals.shape, jnp.float32)

    def vmem(*dims):
        return pltpu.VMEM(dims, jnp.float32)

    orbitals, potential = (
        pltpu.with_memory_space_constraint(a, pltpu.HBM) for a in (orbitals, potential)
    )
    results = pl.pallas_call(
        functools.partial(solve_kernel, sizes),
        out_shape=(shape, shape),
        in_specs=[pl.BlockSpec(memory_space=pltpu.HBM)] * 2,
        out_specs=(pl.BlockSpec(memory_space=pltpu.VMEM),) * 2,
        scratch_shapes=[
            vmem(ROUNDS, 2, count, bx + 2 * HALO, tall, nz),
            vmem(2, bx + 4, tall, nz),
            vmem(POWERS + 1, 2, count, bx, tall, nz),
            vmem(bx + 4, tall, nz),
            vmem(bx + 4, tall, nz),
            vmem(bx + 4, tall, nz),
            vmem(bx + 4, tall, nz),
            vmem(*orbitals.shape),
            vmem(*orbitals.shape),
            vmem(2, count, 8, nz),
            vmem(2, 8, nz),
            vmem(2, devices, 8, nz),
            dma((ROUNDS, count, len(SIDES))),
            dma((ROUNDS, count, len(SIDES))),
            dma((len(SIDES),)),
            dma((len(SIDES),)),
            dma((2, devices)),
            dma((2, devices)),
            dma((count + 1,)),
        ],
        compiler_params=pltpu.CompilerParams(
            collective_id=0, has_side_effects=True, vmem_limit_bytes=VMEM_LIMIT
        ),
    )(orbitals, potential)
    return store(results)


def step(sizes, orbitals, potential):
    _, count, bx, by, nz = orbitals.shape
    near = max(sizes) <= ROUNDS
    fits = (POWERS + 2 * ROUNDS) * count * (bx + 8) * (by + 16) * nz <= 1 << 23
    packs = count <= 8 and (POWERS + 1) ** 2 <= nz
    if near and fits and packs and by % 8 == 0 and nz == 128 and bx >= 4:
        return powers(sizes, orbitals, potential)
    return shards(orbitals, potential)


def solution(mesh):
    sizes = (mesh.shape["gx"], mesh.shape["gyz"])
    return jax.shard_map(
        functools.partial(step, sizes),
        mesh=mesh,
        in_specs=(P(None, "orb", "gx", "gyz", None), P("gx", "gyz", None)),
        out_specs=(P(None, "orb", "gx", "gyz", None), P(None, "orb", "gx", "gyz", None)),
        check_vma=False,
    )
```

```python
import functools

import jax
import jax.numpy as jnp
from jax import lax
from jax.experimental import pallas as pl
from jax.experimental.pallas import tpu as pltpu
from jax.sharding import PartitionSpec as P

ITERS = 4


SPACING = 0.25
HALF_STEP = 0.05
COEFF_NEAR = 4.0 / 3.0
COEFF_FAR = -1.0 / 12.0
COEFF_SELF = -2.5


def with_halo(array, sides, width):
    for axis, dim in sides:
        size, length = (lax.axis_size(axis), array.shape[dim])
        up = [(i, (i + 1) % size) for i in range(size - 1)]
        down = [(j, i) for i, j in up]
        last = lax.slice_in_dim(array, length - width, length, axis=dim)
        leading = lax.slice_in_dim(array, 0, width, axis=dim)
        before = lax.ppermute(last, axis, up)
        after = lax.ppermute(leading, axis, down)
        array = jnp.concatenate([before, array, after], axis=dim)
    return array


def laplace_apply(padded, potential):
    extent = (padded.shape[2] - 4, padded.shape[3] - 4, padded.shape[4] - 4)

    def window(shift_x, shift_y, shift_z):
        return padded[
            :,
            :,
            2 + shift_x : 2 + shift_x + extent[0],
            2 + shift_y : 2 + shift_y + extent[1],
            2 + shift_z : 2 + shift_z + extent[2],
        ]

    center = window(0, 0, 0)
    summed = 3.0 * COEFF_SELF * center
    for offset, weight in ((1, COEFF_NEAR), (2, COEFF_FAR)):
        summed = summed + weight * (
            window(offset, 0, 0)
            + window(-offset, 0, 0)
            + window(0, offset, 0)
            + window(0, -offset, 0)
            + window(0, 0, offset)
            + window(0, 0, -offset)
        )
    return -0.5 / SPACING**2 * summed + potential * center


def pad_depth(vector):
    return jnp.pad(vector, ((0, 0), (0, 0), (0, 0), (0, 0), (2, 2)))


def system(vector, applied):
    return jnp.stack([vector[0] - HALF_STEP * applied[1], vector[1] + HALF_STEP * applied[0]])


def precondition(vector, potential):
    diagonal = HALF_STEP * (3.75 / SPACING**2 + potential)
    divisor = 1.0 + diagonal * diagonal
    return jnp.stack(
        [(vector[0] + diagonal * vector[1]) / divisor, (vector[1] - diagonal * vector[0]) / divisor]
    )


def braket(left, right):
    real_part = jnp.sum(left[0] * right[0] + left[1] * right[1], axis=(1, 2, 3))
    imag_part = jnp.sum(left[0] * right[1] - left[1] * right[0], axis=(1, 2, 3))
    return (real_part, imag_part)


def times_complex(first, second):
    return (
        first[0] * second[0] - first[1] * second[1],
        first[0] * second[1] + first[1] * second[0],
    )


def divide_complex(first, second):
    modulus = second[0] * second[0] + second[1] * second[1]
    return (
        (first[0] * second[0] + first[1] * second[1]) / modulus,
        (first[1] * second[0] - first[0] * second[1]) / modulus,
    )


def scale_complex(coeff, vector):
    real_coef = coeff[0][:, None, None, None]
    imag_coef = coeff[1][:, None, None, None]
    return jnp.stack(
        [
            real_coef * vector[0] - imag_coef * vector[1],
            real_coef * vector[1] + imag_coef * vector[0],
        ]
    )


def shards(orbitals, potential):

    def apply_shallow(vector):
        padded = with_halo(vector, (("gx", 2), ("gyz", 3)), 2)
        return laplace_apply(pad_depth(padded), potential)

    h_orbitals = apply_shallow(orbitals)
    residual = jnp.stack([2.0 * HALF_STEP * h_orbitals[1], -2.0 * HALF_STEP * h_orbitals[0]])
    evolved = orbitals
    shadow = residual
    direction = residual
    rho_now = lax.psum(braket(shadow, residual), ("gx", "gyz"))
    for iteration in range(ITERS):
        dir_hat = precondition(direction, potential)
        image = system(dir_hat, apply_shallow(dir_hat))
        alpha_step = divide_complex(rho_now, lax.psum(braket(shadow, image), ("gx", "gyz")))
        half_step = residual - scale_complex(alpha_step, image)
        half_hat = precondition(half_step, potential)
        second = system(half_hat, apply_shallow(half_hat))
        cross_local = braket(second, half_step)
        norm_local = jnp.sum(second * second, axis=(0, 2, 3, 4))
        shadow_half = braket(shadow, half_step)
        shadow_second = braket(shadow, second)
        summed = lax.psum(
            (
                cross_local[0],
                cross_local[1],
                norm_local,
                shadow_half[0],
                shadow_half[1],
                shadow_second[0],
                shadow_second[1],
            ),
            ("gx", "gyz"),
        )
        cross_real, cross_imag, norm_second = (summed[0], summed[1], summed[2])
        omega_step = (cross_real / norm_second, cross_imag / norm_second)
        evolved = evolved + scale_complex(alpha_step, dir_hat) + scale_complex(omega_step, half_hat)
        residual = half_step - scale_complex(omega_step, second)
        if iteration + 1 < ITERS:
            along_second = times_complex(omega_step, (summed[5], summed[6]))
            rho_next = (summed[3] - along_second[0], summed[4] - along_second[1])
            beta_step = times_complex(
                divide_complex(rho_next, rho_now), divide_complex(alpha_step, omega_step)
            )
            direction = residual + scale_complex(
                beta_step, direction - scale_complex(omega_step, image)
            )
            rho_now = rho_next
    return (evolved, residual)


UNROLL = 16
LEAD = 8
HALO = 4
VMEM_LIMIT = 48000000
LATER_NS = 1000
POWERS = 2 * ITERS
ROUNDS = ITERS + 1
NEAR = -0.5 / SPACING**2 * COEFF_NEAR * HALF_STEP
FAR = -0.5 / SPACING**2 * COEFF_FAR * HALF_STEP
SIDES = ((0, -1), (0, 1), (-1, -1), (-1, 1), (1, -1), (1, 1), (-1, 0), (1, 0))


def sweep(count, plane, carry, unroll=UNROLL):
    width = unroll if count % unroll == 0 else 1

    def group(i, carry):
        for k in range(width):
            carry = plane(i * width + k, carry)
        return carry

    return lax.fori_loop(0, count // width, group, carry)


def power(vector):
    zero = jnp.zeros_like(vector[0][0])
    padded = vector + [(zero, zero)]
    out = [padded[0]]
    for j in range(1, len(padded)):
        out.append((padded[j][0] + padded[j - 1][0], padded[j][1] + padded[j - 1][1]))
    return out


def add_scaled(base, scale, vector):
    out = []
    for j in range(max(len(base), len(vector))):
        if j >= len(vector):
            out.append(base[j])
            continue
        term = times_complex(scale, vector[j])
        out.append((base[j][0] + term[0], base[j][1] + term[1]) if j < len(base) else term)
    return out


def negated(value):
    return (-value[0], -value[1])


def plus(first, second):
    if first is None:
        return second
    return (first[0] + second[0], first[1] + second[1])


def conj_times(first, second):
    return (
        first[0] * second[0] + first[1] * second[1],
        first[0] * second[1] - first[1] * second[0],
    )


def conj_dot(left, right):
    total = None
    for a, b in zip(left, right):
        total = plus(total, conj_times(a, b))
    return total


def recurrence(gram):
    def times_gram(i, vector):
        total = None
        for j, value in enumerate(vector):
            total = plus(total, times_complex(gram(i, j), value))
        return total

    one = jnp.ones_like(gram(0, 0)[0])
    unit = [(one, jnp.zeros_like(one))]
    residual, direction, change = unit, unit, []
    rho = times_gram(0, residual)
    for iteration in range(ITERS):
        image = power(direction)
        alpha = divide_complex(rho, times_gram(0, image))
        half = add_scaled(residual, negated(alpha), image)
        second = power(half)
        change = add_scaled(change, alpha, direction)
        if iteration + 1 == ITERS:
            known = [times_gram(i, second[:-1]) for i in range(len(half))]
            cross = conj_dot(half, known)
            norm = conj_dot(second[:-1], known)[0]
            return change, half, second, cross, norm
        applied = [times_gram(i, second) for i in range(len(second))]
        cross = conj_dot(half, applied)
        norm = conj_dot(second, applied)[0]
        omega = (cross[0] / norm, -cross[1] / norm)
        change = add_scaled(change, omega, half)
        residual = add_scaled(half, negated(omega), second)
        rho_next = times_gram(0, residual)
        beta = times_complex(divide_complex(rho_next, rho), divide_complex(alpha, omega))
        inner = add_scaled(direction, negated(omega), image)
        direction = add_scaled(residual, beta, inner)
        rho = rho_next


def closing(column, half, second, cross, norm):
    top = second[-1]
    along = times_complex(top, conj_dot(half, column))
    cross = plus(cross, along)
    across = times_complex(top, conj_dot(second[:-1], column))
    norm = norm + 2.0 * across[0] + (top[0] * top[0] + top[1] * top[1]) * column[-1][0]
    return (cross[0] / norm, -cross[1] / norm)


def solve_kernel(
    sizes,
    orb_hbm,
    pot_hbm,
    evolved_ref,
    residual_ref,
    fields,
    inner,
    basis,
    pot,
    diag,
    quot,
    quot_d,
    second_ref,
    hat_ref,
    partial,
    gram_own,
    gram_all,
    send_sem,
    recv_sem,
    send_pot,
    recv_pot,
    send_gram,
    recv_gram,
    local_sem,
):
    size_x, size_y = sizes
    count, bx, by, nz = evolved_ref.shape[1:]
    gx, gy = (lax.axis_index("gx"), lax.axis_index("gyz"))
    me = gx * size_y + gy
    devices = size_x * size_y
    rows = slice(LEAD, LEAD + by)
    planes = slice(HALO, HALO + bx)

    def has(dx, dy):
        x, y = (gx + dx, gy + dy)
        inside = jnp.logical_and(x >= 0, x < size_x)
        return jnp.logical_and(inside, jnp.logical_and(y >= 0, y < size_y))

    def loads(o):
        return pltpu.make_async_copy(
            orb_hbm.at[:, o], fields.at[0, :, o, planes, rows, :], local_sem.at[o]
        )

    load_pot = pltpu.make_async_copy(
        pot_hbm, pot.at[pl.ds(2, bx), pl.ds(LEAD, by), :], local_sem.at[count]
    )
    load_pot.start()
    for o in range(count):
        loads(o).start()

    barrier = pltpu.get_barrier_semaphore()
    partners = 0
    for dx, dy in SIDES:
        there = has(dx, dy)
        partners = partners + there.astype(jnp.int32)

        @pl.when(there)
        def _():
            pl.semaphore_signal(
                barrier,
                inc=1,
                device_id={"gx": gx + dx, "gyz": gy + dy},
                device_id_type=pl.DeviceIdType.MESH,
            )

    def spans(d, first, extent, depth):
        if d == 0:
            return (pl.ds(first, extent), pl.ds(first, extent))
        if d > 0:
            return (pl.ds(first + extent - depth, depth), pl.ds(first - depth, depth))
        return (pl.ds(first, depth), pl.ds(first + extent, depth))

    def remote(src, dst, send, recv, dx, dy):
        return pltpu.make_async_remote_copy(
            src_ref=src,
            dst_ref=dst,
            send_sem=send,
            recv_sem=recv,
            device_id={"gx": gx + dx, "gyz": gy + dy},
            device_id_type=pl.DeviceIdType.MESH,
        )

    def halo_copy(r, o, k):
        dx, dy = SIDES[k]
        depth = 2 if (r == ROUNDS - 1 or (dx and dy)) else HALO
        sx, tx = spans(dx, HALO, bx, depth)
        sy, ty = spans(dy, LEAD, by, depth)
        return remote(
            fields.at[r, :, o, sx, sy, :],
            fields.at[r, :, o, tx, ty, :],
            send_sem.at[r, o, k],
            recv_sem.at[r, o, k],
            dx,
            dy,
        )

    def pot_copy(k):
        dx, dy = SIDES[k]
        sx, tx = spans(dx, 2, bx, 2)
        sy, ty = spans(dy, LEAD, by, 2)
        return remote(
            pot.at[sx, sy, :], pot.at[tx, ty, :], send_pot.at[k], recv_pot.at[k], dx, dy
        )

    def straight(k):
        return SIDES[k][0] == 0 or SIDES[k][1] == 0

    def ways(r):
        return [k for k in range(len(SIDES)) if r < ROUNDS - 1 or straight(k)]

    def send_halo(r, o):
        for k in ways(r):
            @pl.when(has(*SIDES[k]))
            def _():
                halo_copy(r, o, k).start()

    def wait_halo(r, o):
        for k in ways(r):
            @pl.when(has(-SIDES[k][0], -SIDES[k][1]))
            def _():
                halo_copy(r, o, k).wait_recv()

    def clear_edges(ref, halo):
        width, height = ref.shape[-3:-1]
        lead = ref.shape[:-3]
        flat = [()]
        for extent in lead:
            flat = [index + (i,) for index in flat for i in range(extent)]
        low, high = (LEAD - HALO, LEAD + by)

        def side(edge, first, stop):
            @pl.when(edge)
            def _():
                def clear(x, carry):
                    for index in flat:
                        ref[index + (x,)] = jnp.zeros((height, nz), jnp.float32)
                    return carry

                lax.fori_loop(first, stop, clear, 0)

        def band(edge, start):
            @pl.when(edge)
            def _():
                def clear(x, carry):
                    for index in flat:
                        ref[index + (x, slice(start, start + HALO))] = jnp.zeros(
                            (HALO, nz), jnp.float32
                        )
                    return carry

                lax.fori_loop(0, width, clear, 0)

        side(gx == 0, 0, halo)
        side(gx == size_x - 1, width - halo, width)
        band(gy == 0, low)
        band(gy == size_y - 1, high)

    clear_edges(pot, 2)
    clear_edges(fields.at[0], HALO)

    pl.semaphore_wait(barrier, partners)
    load_pot.wait()
    for k in range(len(SIDES)):
        if straight(k):
            @pl.when(has(*SIDES[k]))
            def _():
                pot_copy(k).start()
    for o in range(count):
        loads(o).wait()
    late = lax.axis_index("orb") % 2 == 1

    def send_first():
        for o in range(count):
            send_halo(0, o)

    pl.when(jnp.logical_not(late))(send_first)

    for r in range(1, ROUNDS):
        clear_edges(fields.at[r], HALO)
    for o in range(count):
        for half in range(2):
            partial[half, o] = jnp.zeros((8, nz), jnp.float32)

    for k in range(len(SIDES)):
        if straight(k):
            @pl.when(has(-SIDES[k][0], -SIDES[k][1]))
            def _():
                pot_copy(k).wait_recv()

    def hold_then_send():
        pl.delay(LATER_NS)
        send_first()

    pl.when(late)(hold_then_send)

    starts = list(range(-2, by - 5, 8))
    if starts[-1] != by - 6:
        starts.append(by - 6)

    def prepare(x, carry):
        for start in starts:
            span = slice(LEAD + start, LEAD + start + 8)
            d = HALF_STEP * (-1.5 * COEFF_SELF / SPACING**2 + pot[x, span, :])
            q = NEAR / (1.0 + d * d)
            diag[x, span, :] = d
            quot[x, span, :] = q
            quot_d[x, span, :] = q * d
        return carry

    sweep(bx + 4, prepare, 0, bx + 4)
    for ref in (quot, quot_d):
        clear_edges(ref, 2)

    lane = lax.broadcasted_iota(jnp.int32, (8, nz), 1)

    def offdiagonal(ref, x, y):
        def at(dx, dy):
            return ref[x + dx, y + dy : y + dy + 8, :]

        center = at(0, 0)
        near = (at(1, 0) + at(-1, 0)) + (at(0, 1) + at(0, -1))
        far = (at(2, 0) + at(-2, 0)) + (at(0, 2) + at(0, -2))
        near = near + (
            jnp.where(lane < 1, 0.0, pltpu.roll(center, 1, 1))
            + jnp.where(lane >= nz - 1, 0.0, pltpu.roll(center, nz - 1, 1))
        )
        far = far + (
            jnp.where(lane < 2, 0.0, pltpu.roll(center, 2, 1))
            + jnp.where(lane >= nz - 2, 0.0, pltpu.roll(center, nz - 2, 1))
        )
        return near + (FAR / NEAR) * far, center

    def started(r, o, x, y):
        off_re, re = offdiagonal(fields.at[r, 0, o], x + HALO, LEAD + y)
        off_im, im = offdiagonal(fields.at[r, 1, o], x + HALO, LEAD + y)
        d = diag[x + 2, LEAD + y : LEAD + y + 8, :]
        return 2.0 * (NEAR * off_im + d * im), -2.0 * (NEAR * off_re + d * re)

    def outer(r, o, x, y):
        off_re, _ = offdiagonal(fields.at[r, 0, o], x + HALO, LEAD + y)
        off_im, _ = offdiagonal(fields.at[r, 1, o], x + HALO, LEAD + y)
        return -off_im, off_re

    def hats(x, y, re, im):
        span = slice(LEAD + y, LEAD + y + 8)
        q, qd = (quot[x + 2, span, :], quot_d[x + 2, span, :])
        return q * re + qd * im, q * im - qd * re

    def first_stage(r, o):
        apply = started if r == 0 else outer

        def plane(x, carry):
            for y in starts:
                span = slice(LEAD + y, LEAD + y + 8)
                re, im = apply(r, o, x, y)
                basis[2 * r, 0, o, x, span, :] = re
                basis[2 * r, 1, o, x, span, :] = im
                hat_re, hat_im = hats(x, y, re, im)
                inner[0, x + 2, span, :] = hat_re
                inner[1, x + 2, span, :] = hat_im
            return carry

        for x in (-2, -1, bx, bx + 1):
            for y in range(0, by, 8):
                span = slice(LEAD + y, LEAD + y + 8)
                re, im = apply(r, o, x, y)
                hat_re, hat_im = hats(x, y, re, im)
                inner[0, x + 2, span, :] = hat_re
                inner[1, x + 2, span, :] = hat_im
        sweep(bx, plane, 0)

    def second_stage(r, o):
        def plane(x, carry):
            for y in range(0, by, 8):
                span = slice(LEAD + y, LEAD + y + 8)
                off_re, _ = offdiagonal(inner.at[0], x + 2, LEAD + y)
                off_im, _ = offdiagonal(inner.at[1], x + 2, LEAD + y)
                re, im = -off_im, off_re
                basis[2 * r + 1, 0, o, x, span, :] = re
                basis[2 * r + 1, 1, o, x, span, :] = im
                hat_re, hat_im = hats(x, y, re, im)
                fields[r + 1, 0, o, x + HALO, span, :] = hat_re
                fields[r + 1, 1, o, x + HALO, span, :] = hat_im
            return carry

        sweep(bx, plane, 0)

    def last_stage(r, o):
        def plane(x, carry):
            for y in range(0, by, 8):
                span = slice(LEAD + y, LEAD + y + 8)
                re, im = outer(r, o, x, y)
                basis[2 * r, 0, o, x, span, :] = re
                basis[2 * r, 1, o, x, span, :] = im
            return carry

        sweep(bx, plane, 0)

    size = POWERS + 1
    zero = jnp.zeros((8, nz), jnp.float32)

    def products(j, o):
        def plane(x, sums):
            sums = list(sums)
            for y in range(0, by, 8):
                span = slice(LEAD + y, LEAD + y + 8)
                b_re, b_im = (basis[j, 0, o, x, span, :], basis[j, 1, o, x, span, :])
                for i in range(j):
                    a_re, a_im = (basis[i, 0, o, x, span, :], basis[i, 1, o, x, span, :])
                    sums[2 * i] = sums[2 * i] + (a_re * b_re + a_im * b_im)
                    sums[2 * i + 1] = sums[2 * i + 1] + (a_re * b_im - a_im * b_re)
                sums[2 * j] = sums[2 * j] + (b_re * b_re + b_im * b_im)
            return tuple(sums)

        sums = sweep(bx, plane, (zero,) * (2 * j + 1))
        half = 0 if j < POWERS else 1
        packed = partial[half, o]
        for i in range(j + 1):
            packed = jnp.where(
                lane == i * size + j, jnp.sum(sums[2 * i], axis=1, keepdims=True), packed
            )
            if i < j:
                packed = jnp.where(
                    lane == j * size + i, jnp.sum(sums[2 * i + 1], axis=1, keepdims=True), packed
                )
        partial[half, o] = packed

    row = lax.broadcasted_iota(jnp.int32, (8, nz), 0)

    def gram_copy(half, dev, x, y):
        return pltpu.make_async_remote_copy(
            src_ref=gram_own.at[half, 0:count],
            dst_ref=gram_all.at[half, dev, 0:count],
            send_sem=send_gram.at[half, x * size_y + y],
            recv_sem=recv_gram.at[half, dev],
            device_id={"gx": x, "gyz": y},
            device_id_type=pl.DeviceIdType.MESH,
        )

    def share(half):
        packed = zero
        for o in range(count):
            packed = jnp.where(
                row == o, jnp.sum(partial[half, o], axis=0, keepdims=True), packed
            )
        gram_own[half] = packed
        gram_all[half, pl.ds(me, 1)] = packed[None]
        for dev in range(devices):
            @pl.when(me != dev)
            def _():
                gram_copy(half, me, dev // size_y, dev % size_y).start()

    def shared(half):
        for dev in range(devices):
            @pl.when(me != dev)
            def _():
                gram_copy(half, dev, gx, gy).wait_recv()

        summed = gram_all[half, 0]
        for dev in range(1, devices):
            summed = summed + gram_all[half, dev]
        summed = jnp.where(row < count, summed, 1.0)
        values = {}

        def spread(index):
            return jnp.broadcast_to(summed[:, index : index + 1], (8, nz))

        def gram(i, j):
            if i > j:
                re, im = gram(j, i)
                return re, -im
            if (i, j) not in values:
                re = spread(i * size + j)
                values[i, j] = (re, spread(j * size + i) if i < j else jnp.zeros_like(re))
            return values[i, j]

        return gram

    for r in range(ROUNDS):
        last = r == ROUNDS - 1

        def advance(o, carry):
            wait_halo(r, o)
            if last:
                last_stage(r, o)
                products(2 * r, o)
            else:
                first_stage(r, o)
                second_stage(r, o)
                send_halo(r + 1, o)
            return carry

        lax.fori_loop(0, count, advance, 0)
        if last:
            share(1)
        else:
            def gather(o, carry):
                products(2 * r, o)
                products(2 * r + 1, o)
                return carry

            lax.fori_loop(0, count, gather, 0)
            if r == ROUNDS - 2:
                share(0)

    change, halved, doubled, cross, norm = recurrence(shared(0))
    change = [(a / NEAR, b / NEAR) for a, b in change]

    def combine(o, x, span, coefs):
        total = None
        for j, c in enumerate(coefs):
            term = times_complex(c, (basis[j, 0, o, x, span, :], basis[j, 1, o, x, span, :]))
            total = plus(total, term)
        return total

    for o in range(count):
        def own(values):
            return [
                tuple(jnp.broadcast_to(part[o : o + 1], (8, nz)) for part in value)
                for value in values
            ]

        moves, halves, seconds = (own(change), own(halved), own(doubled))

        def blend(x, carry):
            for y in range(0, by, 8):
                span = slice(LEAD + y, LEAD + y + 8)
                out = slice(y, y + 8)
                for ref, total in (
                    (residual_ref, combine(o, x, span, halves)),
                    (second_ref, combine(o, x, span, seconds)),
                ):
                    ref[0, o, x, out, :] = total[0]
                    ref[1, o, x, out, :] = total[1]
                hat = hats(x, y, residual_ref[0, o, x, out, :], residual_ref[1, o, x, out, :])
                hat_ref[0, o, x, out, :] = hat[0]
                hat_ref[1, o, x, out, :] = hat[1]
                hat = hats(x, y, *combine(o, x, span, moves))
                evolved_ref[0, o, x, out, :] = fields[0, 0, o, x + HALO, span, :] + hat[0]
                evolved_ref[1, o, x, out, :] = fields[0, 1, o, x + HALO, span, :] + hat[1]
            return carry

        sweep(bx, blend, 0)

    for k in range(len(SIDES)):
        @pl.when(has(*SIDES[k]))
        def _():
            if straight(k):
                pot_copy(k).wait_send()
            for r in range(ROUNDS):
                if k in ways(r):
                    for o in range(count):
                        halo_copy(r, o, k).wait_send()

    gram = shared(1)
    column = [gram(i, POWERS) for i in range(size)]
    omega = closing(column, halved, doubled, cross, norm)
    scaled = (omega[0] / NEAR, omega[1] / NEAR)

    for o in range(count):
        step_r, step_e = (
            tuple(jnp.broadcast_to(part[o : o + 1], (8, nz)) for part in value)
            for value in (omega, scaled)
        )

        def finish(x, carry):
            for y in range(0, by, 8):
                out = slice(y, y + 8)
                for ref, other, coef, sign in (
                    (residual_ref, second_ref, step_r, -1.0),
                    (evolved_ref, hat_ref, step_e, 1.0),
                ):
                    term = times_complex(coef, (other[0, o, x, out, :], other[1, o, x, out, :]))
                    ref[0, o, x, out, :] = ref[0, o, x, out, :] + sign * term[0]
                    ref[1, o, x, out, :] = ref[1, o, x, out, :] + sign * term[1]
            return carry

        sweep(bx, finish, 0)

    for half in range(2):
        for dev in range(devices):
            @pl.when(me != dev)
            def _():
                gram_copy(half, me, dev // size_y, dev % size_y).wait_send()


def store_kernel(count, *refs):
    sources, targets, sems = (refs[:count], refs[count : 2 * count], refs[-1])
    copies = [
        pltpu.make_async_copy(sources[k], targets[k], sems.at[k]) for k in range(count)
    ]
    for copy in copies:
        copy.start()
    for copy in copies:
        copy.wait()


def store(arrays):
    count = len(arrays)
    return pl.pallas_call(
        functools.partial(store_kernel, count),
        out_shape=tuple(jax.ShapeDtypeStruct(a.shape, a.dtype) for a in arrays),
        in_specs=[pl.BlockSpec(memory_space=pltpu.VMEM)] * count,
        out_specs=(pl.BlockSpec(memory_space=pltpu.HBM),) * count,
        scratch_shapes=[pltpu.SemaphoreType.DMA((count,))],
        compiler_params=pltpu.CompilerParams(vmem_limit_bytes=1 << 20),
    )(*arrays)


def powers(sizes, orbitals, potential):
    size_x, size_y = sizes
    _, count, bx, by, nz = orbitals.shape
    tall = by + 2 * LEAD
    devices = size_x * size_y
    dma = pltpu.SemaphoreType.DMA
    shape = jax.ShapeDtypeStruct(orbitals.shape, jnp.float32)

    def vmem(*dims):
        return pltpu.VMEM(dims, jnp.float32)

    orbitals, potential = (
        pltpu.with_memory_space_constraint(a, pltpu.HBM) for a in (orbitals, potential)
    )
    results = pl.pallas_call(
        functools.partial(solve_kernel, sizes),
        out_shape=(shape, shape),
        in_specs=[pl.BlockSpec(memory_space=pltpu.HBM)] * 2,
        out_specs=(pl.BlockSpec(memory_space=pltpu.VMEM),) * 2,
        scratch_shapes=[
            vmem(ROUNDS, 2, count, bx + 2 * HALO, tall, nz),
            vmem(2, bx + 4, tall, nz),
            vmem(POWERS + 1, 2, count, bx, tall, nz),
            vmem(bx + 4, tall, nz),
            vmem(bx + 4, tall, nz),
            vmem(bx + 4, tall, nz),
            vmem(bx + 4, tall, nz),
            vmem(*orbitals.shape),
            vmem(*orbitals.shape),
            vmem(2, count, 8, nz),
            vmem(2, 8, nz),
            vmem(2, devices, 8, nz),
            dma((ROUNDS, count, len(SIDES))),
            dma((ROUNDS, count, len(SIDES))),
            dma((len(SIDES),)),
            dma((len(SIDES),)),
            dma((2, devices)),
            dma((2, devices)),
            dma((count + 1,)),
        ],
        compiler_params=pltpu.CompilerParams(
            collective_id=0, has_side_effects=True, vmem_limit_bytes=VMEM_LIMIT
        ),
    )(orbitals, potential)
    return store(results)


def step(sizes, orbitals, potential):
    _, count, bx, by, nz = orbitals.shape
    near = max(sizes) <= ROUNDS
    fits = (POWERS + 2 * ROUNDS) * count * (bx + 8) * (by + 16) * nz <= 1 << 23
    packs = count <= 8 and (POWERS + 1) ** 2 <= nz
    if near and fits and packs and by % 8 == 0 and nz == 128 and bx >= 4:
        return powers(sizes, orbitals, potential)
    return shards(orbitals, potential)


def solution(mesh):
    sizes = (mesh.shape["gx"], mesh.shape["gyz"])
    return jax.shard_map(
        functools.partial(step, sizes),
        mesh=mesh,
        in_specs=(P(None, "orb", "gx", "gyz", None), P("gx", "gyz", None)),
        out_specs=(P(None, "orb", "gx", "gyz", None), P(None, "orb", "gx", "gyz", None)),
        check_vma=False,
    )
```

```python
import functools

import jax
import jax.numpy as jnp
from jax import lax
from jax.experimental import pallas as pl
from jax.experimental.pallas import tpu as pltpu
from jax.sharding import PartitionSpec as P

ITERS = 4


SPACING = 0.25
HALF_STEP = 0.05
COEFF_NEAR = 4.0 / 3.0
COEFF_FAR = -1.0 / 12.0
COEFF_SELF = -2.5


def with_halo(array, sides, width):
    for axis, dim in sides:
        size, length = (lax.axis_size(axis), array.shape[dim])
        up = [(i, (i + 1) % size) for i in range(size - 1)]
        down = [(j, i) for i, j in up]
        last = lax.slice_in_dim(array, length - width, length, axis=dim)
        leading = lax.slice_in_dim(array, 0, width, axis=dim)
        before = lax.ppermute(last, axis, up)
        after = lax.ppermute(leading, axis, down)
        array = jnp.concatenate([before, array, after], axis=dim)
    return array


def laplace_apply(padded, potential):
    extent = (padded.shape[2] - 4, padded.shape[3] - 4, padded.shape[4] - 4)

    def window(shift_x, shift_y, shift_z):
        return padded[
            :,
            :,
            2 + shift_x : 2 + shift_x + extent[0],
            2 + shift_y : 2 + shift_y + extent[1],
            2 + shift_z : 2 + shift_z + extent[2],
        ]

    center = window(0, 0, 0)
    summed = 3.0 * COEFF_SELF * center
    for offset, weight in ((1, COEFF_NEAR), (2, COEFF_FAR)):
        summed = summed + weight * (
            window(offset, 0, 0)
            + window(-offset, 0, 0)
            + window(0, offset, 0)
            + window(0, -offset, 0)
            + window(0, 0, offset)
            + window(0, 0, -offset)
        )
    return -0.5 / SPACING**2 * summed + potential * center


def pad_depth(vector):
    return jnp.pad(vector, ((0, 0), (0, 0), (0, 0), (0, 0), (2, 2)))


def system(vector, applied):
    return jnp.stack([vector[0] - HALF_STEP * applied[1], vector[1] + HALF_STEP * applied[0]])


def precondition(vector, potential):
    diagonal = HALF_STEP * (3.75 / SPACING**2 + potential)
    divisor = 1.0 + diagonal * diagonal
    return jnp.stack(
        [(vector[0] + diagonal * vector[1]) / divisor, (vector[1] - diagonal * vector[0]) / divisor]
    )


def braket(left, right):
    real_part = jnp.sum(left[0] * right[0] + left[1] * right[1], axis=(1, 2, 3))
    imag_part = jnp.sum(left[0] * right[1] - left[1] * right[0], axis=(1, 2, 3))
    return (real_part, imag_part)


def times_complex(first, second):
    return (
        first[0] * second[0] - first[1] * second[1],
        first[0] * second[1] + first[1] * second[0],
    )


def divide_complex(first, second):
    modulus = second[0] * second[0] + second[1] * second[1]
    return (
        (first[0] * second[0] + first[1] * second[1]) / modulus,
        (first[1] * second[0] - first[0] * second[1]) / modulus,
    )


def scale_complex(coeff, vector):
    real_coef = coeff[0][:, None, None, None]
    imag_coef = coeff[1][:, None, None, None]
    return jnp.stack(
        [
            real_coef * vector[0] - imag_coef * vector[1],
            real_coef * vector[1] + imag_coef * vector[0],
        ]
    )


def shards(orbitals, potential):

    def apply_shallow(vector):
        padded = with_halo(vector, (("gx", 2), ("gyz", 3)), 2)
        return laplace_apply(pad_depth(padded), potential)

    h_orbitals = apply_shallow(orbitals)
    residual = jnp.stack([2.0 * HALF_STEP * h_orbitals[1], -2.0 * HALF_STEP * h_orbitals[0]])
    evolved = orbitals
    shadow = residual
    direction = residual
    rho_now = lax.psum(braket(shadow, residual), ("gx", "gyz"))
    for iteration in range(ITERS):
        dir_hat = precondition(direction, potential)
        image = system(dir_hat, apply_shallow(dir_hat))
        alpha_step = divide_complex(rho_now, lax.psum(braket(shadow, image), ("gx", "gyz")))
        half_step = residual - scale_complex(alpha_step, image)
        half_hat = precondition(half_step, potential)
        second = system(half_hat, apply_shallow(half_hat))
        cross_local = braket(second, half_step)
        norm_local = jnp.sum(second * second, axis=(0, 2, 3, 4))
        shadow_half = braket(shadow, half_step)
        shadow_second = braket(shadow, second)
        summed = lax.psum(
            (
                cross_local[0],
                cross_local[1],
                norm_local,
                shadow_half[0],
                shadow_half[1],
                shadow_second[0],
                shadow_second[1],
            ),
            ("gx", "gyz"),
        )
        cross_real, cross_imag, norm_second = (summed[0], summed[1], summed[2])
        omega_step = (cross_real / norm_second, cross_imag / norm_second)
        evolved = evolved + scale_complex(alpha_step, dir_hat) + scale_complex(omega_step, half_hat)
        residual = half_step - scale_complex(omega_step, second)
        if iteration + 1 < ITERS:
            along_second = times_complex(omega_step, (summed[5], summed[6]))
            rho_next = (summed[3] - along_second[0], summed[4] - along_second[1])
            beta_step = times_complex(
                divide_complex(rho_next, rho_now), divide_complex(alpha_step, omega_step)
            )
            direction = residual + scale_complex(
                beta_step, direction - scale_complex(omega_step, image)
            )
            rho_now = rho_next
    return (evolved, residual)


UNROLL = 16
LEAD = 8
HALO = 4
VMEM_LIMIT = 48000000
LATER_NS = 1000
POWERS = 2 * ITERS
ROUNDS = ITERS + 1
NEAR = -0.5 / SPACING**2 * COEFF_NEAR * HALF_STEP
FAR = -0.5 / SPACING**2 * COEFF_FAR * HALF_STEP
SIDES = ((0, -1), (0, 1), (-1, -1), (-1, 1), (1, -1), (1, 1), (-1, 0), (1, 0))


def sweep(count, plane, carry, unroll=UNROLL):
    width = unroll if count % unroll == 0 else 1

    def group(i, carry):
        for k in range(width):
            carry = plane(i * width + k, carry)
        return carry

    return lax.fori_loop(0, count // width, group, carry)


def power(vector):
    zero = jnp.zeros_like(vector[0][0])
    padded = vector + [(zero, zero)]
    out = [padded[0]]
    for j in range(1, len(padded)):
        out.append((padded[j][0] + padded[j - 1][0], padded[j][1] + padded[j - 1][1]))
    return out


def add_scaled(base, scale, vector):
    out = []
    for j in range(max(len(base), len(vector))):
        if j >= len(vector):
            out.append(base[j])
            continue
        term = times_complex(scale, vector[j])
        out.append((base[j][0] + term[0], base[j][1] + term[1]) if j < len(base) else term)
    return out


def negated(value):
    return (-value[0], -value[1])


def plus(first, second):
    if first is None:
        return second
    return (first[0] + second[0], first[1] + second[1])


def conj_times(first, second):
    return (
        first[0] * second[0] + first[1] * second[1],
        first[0] * second[1] - first[1] * second[0],
    )


def conj_dot(left, right):
    total = None
    for a, b in zip(left, right):
        total = plus(total, conj_times(a, b))
    return total


def recurrence(gram):
    def times_gram(i, vector):
        total = None
        for j, value in enumerate(vector):
            total = plus(total, times_complex(gram(i, j), value))
        return total

    one = jnp.ones_like(gram(0, 0)[0])
    unit = [(one, jnp.zeros_like(one))]
    residual, direction, change = unit, unit, []
    rho = times_gram(0, residual)
    for iteration in range(ITERS):
        image = power(direction)
        alpha = divide_complex(rho, times_gram(0, image))
        half = add_scaled(residual, negated(alpha), image)
        second = power(half)
        change = add_scaled(change, alpha, direction)
        if iteration + 1 == ITERS:
            known = [times_gram(i, second[:-1]) for i in range(len(half))]
            cross = conj_dot(half, known)
            norm = conj_dot(second[:-1], known)[0]
            return change, half, second, cross, norm
        applied = [times_gram(i, second) for i in range(len(second))]
        cross = conj_dot(half, applied)
        norm = conj_dot(second, applied)[0]
        omega = (cross[0] / norm, -cross[1] / norm)
        change = add_scaled(change, omega, half)
        residual = add_scaled(half, negated(omega), second)
        rho_next = times_gram(0, residual)
        beta = times_complex(divide_complex(rho_next, rho), divide_complex(alpha, omega))
        inner = add_scaled(direction, negated(omega), image)
        direction = add_scaled(residual, beta, inner)
        rho = rho_next


def closing(column, half, second, cross, norm):
    top = second[-1]
    along = times_complex(top, conj_dot(half, column))
    cross = plus(cross, along)
    across = times_complex(top, conj_dot(second[:-1], column))
    norm = norm + 2.0 * across[0] + (top[0] * top[0] + top[1] * top[1]) * column[-1][0]
    return (cross[0] / norm, -cross[1] / norm)


def solve_kernel(
    sizes,
    orb_hbm,
    pot_hbm,
    evolved_ref,
    residual_ref,
    fields,
    inner,
    basis,
    pot,
    diag,
    quot,
    quot_d,
    second_ref,
    hat_ref,
    partial,
    gram_own,
    gram_all,
    send_sem,
    recv_sem,
    send_pot,
    recv_pot,
    send_gram,
    recv_gram,
    local_sem,
):
    size_x, size_y = sizes
    count, bx, by, nz = evolved_ref.shape[1:]
    gx, gy = (lax.axis_index("gx"), lax.axis_index("gyz"))
    me = gx * size_y + gy
    devices = size_x * size_y
    rows = slice(LEAD, LEAD + by)
    planes = slice(HALO, HALO + bx)

    def has(dx, dy):
        x, y = (gx + dx, gy + dy)
        inside = jnp.logical_and(x >= 0, x < size_x)
        return jnp.logical_and(inside, jnp.logical_and(y >= 0, y < size_y))

    def loads(o):
        return pltpu.make_async_copy(
            orb_hbm.at[:, o], fields.at[0, :, o, planes, rows, :], local_sem.at[o]
        )

    load_pot = pltpu.make_async_copy(
        pot_hbm, pot.at[pl.ds(2, bx), pl.ds(LEAD, by), :], local_sem.at[count]
    )
    load_pot.start()
    for o in range(count):
        loads(o).start()

    barrier = pltpu.get_barrier_semaphore()
    partners = 0
    for dx, dy in SIDES:
        there = has(dx, dy)
        partners = partners + there.astype(jnp.int32)

        @pl.when(there)
        def _():
            pl.semaphore_signal(
                barrier,
                inc=1,
                device_id={"gx": gx + dx, "gyz": gy + dy},
                device_id_type=pl.DeviceIdType.MESH,
            )

    def spans(d, first, extent, depth):
        if d == 0:
            return (pl.ds(first, extent), pl.ds(first, extent))
        if d > 0:
            return (pl.ds(first + extent - depth, depth), pl.ds(first - depth, depth))
        return (pl.ds(first, depth), pl.ds(first + extent, depth))

    def remote(src, dst, send, recv, dx, dy):
        return pltpu.make_async_remote_copy(
            src_ref=src,
            dst_ref=dst,
            send_sem=send,
            recv_sem=recv,
            device_id={"gx": gx + dx, "gyz": gy + dy},
            device_id_type=pl.DeviceIdType.MESH,
        )

    def halo_copy(r, o, k):
        dx, dy = SIDES[k]
        depth = 2 if (r == ROUNDS - 1 or (dx and dy)) else HALO
        sx, tx = spans(dx, HALO, bx, depth)
        sy, ty = spans(dy, LEAD, by, depth)
        return remote(
            fields.at[r, :, o, sx, sy, :],
            fields.at[r, :, o, tx, ty, :],
            send_sem.at[r, o, k],
            recv_sem.at[r, o, k],
            dx,
            dy,
        )

    def pot_copy(k):
        dx, dy = SIDES[k]
        sx, tx = spans(dx, 2, bx, 2)
        sy, ty = spans(dy, LEAD, by, 2)
        return remote(
            pot.at[sx, sy, :], pot.at[tx, ty, :], send_pot.at[k], recv_pot.at[k], dx, dy
        )

    def straight(k):
        return SIDES[k][0] == 0 or SIDES[k][1] == 0

    def ways(r):
        return [k for k in range(len(SIDES)) if r < ROUNDS - 1 or straight(k)]

    def send_halo(r, o):
        for k in ways(r):
            @pl.when(has(*SIDES[k]))
            def _():
                halo_copy(r, o, k).start()

    def wait_halo(r, o):
        for k in ways(r):
            @pl.when(has(-SIDES[k][0], -SIDES[k][1]))
            def _():
                halo_copy(r, o, k).wait_recv()

    def clear_edges(ref, halo):
        width, height = ref.shape[-3:-1]
        lead = ref.shape[:-3]
        flat = [()]
        for extent in lead:
            flat = [index + (i,) for index in flat for i in range(extent)]
        low, high = (LEAD - HALO, LEAD + by)

        def side(edge, first, stop):
            @pl.when(edge)
            def _():
                def clear(x, carry):
                    for index in flat:
                        ref[index + (x,)] = jnp.zeros((height, nz), jnp.float32)
                    return carry

                lax.fori_loop(first, stop, clear, 0)

        def band(edge, start):
            @pl.when(edge)
            def _():
                def clear(x, carry):
                    for index in flat:
                        ref[index + (x, slice(start, start + HALO))] = jnp.zeros(
                            (HALO, nz), jnp.float32
                        )
                    return carry

                lax.fori_loop(0, width, clear, 0)

        side(gx == 0, 0, halo)
        side(gx == size_x - 1, width - halo, width)
        band(gy == 0, low)
        band(gy == size_y - 1, high)

    clear_edges(pot, 2)
    clear_edges(fields.at[0], HALO)

    pl.semaphore_wait(barrier, partners)
    load_pot.wait()
    for k in range(len(SIDES)):
        if straight(k):
            @pl.when(has(*SIDES[k]))
            def _():
                pot_copy(k).start()
    late = lax.axis_index("orb") % 2 == 1

    def send_first():
        for o in range(count):
            loads(o).wait()
            send_halo(0, o)

    pl.when(jnp.logical_not(late))(send_first)

    for r in range(1, ROUNDS):
        clear_edges(fields.at[r], HALO)
    for o in range(count):
        for half in range(2):
            partial[half, o] = jnp.zeros((8, nz), jnp.float32)

    for k in range(len(SIDES)):
        if straight(k):
            @pl.when(has(-SIDES[k][0], -SIDES[k][1]))
            def _():
                pot_copy(k).wait_recv()

    def hold_then_send():
        pl.delay(LATER_NS)
        send_first()

    pl.when(late)(hold_then_send)

    starts = list(range(-2, by - 5, 8))
    if starts[-1] != by - 6:
        starts.append(by - 6)

    def prepare(x, carry):
        for start in starts:
            span = slice(LEAD + start, LEAD + start + 8)
            d = HALF_STEP * (-1.5 * COEFF_SELF / SPACING**2 + pot[x, span, :])
            q = NEAR / (1.0 + d * d)
            diag[x, span, :] = d
            quot[x, span, :] = q
            quot_d[x, span, :] = q * d
        return carry

    sweep(bx + 4, prepare, 0, bx + 4)
    for ref in (quot, quot_d):
        clear_edges(ref, 2)

    lane = lax.broadcasted_iota(jnp.int32, (8, nz), 1)

    def offdiagonal(ref, x, y):
        def at(dx, dy):
            return ref[x + dx, y + dy : y + dy + 8, :]

        center = at(0, 0)
        near = (at(1, 0) + at(-1, 0)) + (at(0, 1) + at(0, -1))
        far = (at(2, 0) + at(-2, 0)) + (at(0, 2) + at(0, -2))
        near = near + (
            jnp.where(lane < 1, 0.0, pltpu.roll(center, 1, 1))
            + jnp.where(lane >= nz - 1, 0.0, pltpu.roll(center, nz - 1, 1))
        )
        far = far + (
            jnp.where(lane < 2, 0.0, pltpu.roll(center, 2, 1))
            + jnp.where(lane >= nz - 2, 0.0, pltpu.roll(center, nz - 2, 1))
        )
        return near + (FAR / NEAR) * far, center

    def started(r, o, x, y):
        off_re, re = offdiagonal(fields.at[r, 0, o], x + HALO, LEAD + y)
        off_im, im = offdiagonal(fields.at[r, 1, o], x + HALO, LEAD + y)
        d = diag[x + 2, LEAD + y : LEAD + y + 8, :]
        return 2.0 * (NEAR * off_im + d * im), -2.0 * (NEAR * off_re + d * re)

    def outer(r, o, x, y):
        off_re, _ = offdiagonal(fields.at[r, 0, o], x + HALO, LEAD + y)
        off_im, _ = offdiagonal(fields.at[r, 1, o], x + HALO, LEAD + y)
        return -off_im, off_re

    def hats(x, y, re, im):
        span = slice(LEAD + y, LEAD + y + 8)
        q, qd = (quot[x + 2, span, :], quot_d[x + 2, span, :])
        return q * re + qd * im, q * im - qd * re

    def first_stage(r, o):
        apply = started if r == 0 else outer

        def plane(x, carry):
            for y in starts:
                span = slice(LEAD + y, LEAD + y + 8)
                re, im = apply(r, o, x, y)
                basis[2 * r, 0, o, x, span, :] = re
                basis[2 * r, 1, o, x, span, :] = im
                hat_re, hat_im = hats(x, y, re, im)
                inner[0, x + 2, span, :] = hat_re
                inner[1, x + 2, span, :] = hat_im
            return carry

        for x in (-2, -1, bx, bx + 1):
            for y in range(0, by, 8):
                span = slice(LEAD + y, LEAD + y + 8)
                re, im = apply(r, o, x, y)
                hat_re, hat_im = hats(x, y, re, im)
                inner[0, x + 2, span, :] = hat_re
                inner[1, x + 2, span, :] = hat_im
        sweep(bx, plane, 0)

    def second_stage(r, o):
        def plane(x, carry):
            for y in range(0, by, 8):
                span = slice(LEAD + y, LEAD + y + 8)
                off_re, _ = offdiagonal(inner.at[0], x + 2, LEAD + y)
                off_im, _ = offdiagonal(inner.at[1], x + 2, LEAD + y)
                re, im = -off_im, off_re
                basis[2 * r + 1, 0, o, x, span, :] = re
                basis[2 * r + 1, 1, o, x, span, :] = im
                hat_re, hat_im = hats(x, y, re, im)
                fields[r + 1, 0, o, x + HALO, span, :] = hat_re
                fields[r + 1, 1, o, x + HALO, span, :] = hat_im
            return carry

        sweep(bx, plane, 0)

    def last_stage(r, o):
        def plane(x, carry):
            for y in range(0, by, 8):
                span = slice(LEAD + y, LEAD + y + 8)
                re, im = outer(r, o, x, y)
                basis[2 * r, 0, o, x, span, :] = re
                basis[2 * r, 1, o, x, span, :] = im
            return carry

        sweep(bx, plane, 0)

    size = POWERS + 1
    zero = jnp.zeros((8, nz), jnp.float32)

    def products(j, o):
        def plane(x, sums):
            sums = list(sums)
            for y in range(0, by, 8):
                span = slice(LEAD + y, LEAD + y + 8)
                b_re, b_im = (basis[j, 0, o, x, span, :], basis[j, 1, o, x, span, :])
                for i in range(j):
                    a_re, a_im = (basis[i, 0, o, x, span, :], basis[i, 1, o, x, span, :])
                    sums[2 * i] = sums[2 * i] + (a_re * b_re + a_im * b_im)
                    sums[2 * i + 1] = sums[2 * i + 1] + (a_re * b_im - a_im * b_re)
                sums[2 * j] = sums[2 * j] + (b_re * b_re + b_im * b_im)
            return tuple(sums)

        sums = sweep(bx, plane, (zero,) * (2 * j + 1))
        half = 0 if j < POWERS else 1
        packed = partial[half, o]
        for i in range(j + 1):
            packed = jnp.where(
                lane == i * size + j, jnp.sum(sums[2 * i], axis=1, keepdims=True), packed
            )
            if i < j:
                packed = jnp.where(
                    lane == j * size + i, jnp.sum(sums[2 * i + 1], axis=1, keepdims=True), packed
                )
        partial[half, o] = packed

    row = lax.broadcasted_iota(jnp.int32, (8, nz), 0)

    def gram_copy(half, dev, x, y):
        return pltpu.make_async_remote_copy(
            src_ref=gram_own.at[half, 0:count],
            dst_ref=gram_all.at[half, dev, 0:count],
            send_sem=send_gram.at[half, x * size_y + y],
            recv_sem=recv_gram.at[half, dev],
            device_id={"gx": x, "gyz": y},
            device_id_type=pl.DeviceIdType.MESH,
        )

    far_first = [
        (dx, dy)
        for dx in range(1 - size_x, size_x)
        for dy in range(1 - size_y, size_y)
        if dx or dy
    ]
    far_first.sort(key=lambda d: -abs(d[0]) - abs(d[1]))

    def share(half):
        packed = zero
        for o in range(count):
            packed = jnp.where(
                row == o, jnp.sum(partial[half, o], axis=0, keepdims=True), packed
            )
        gram_own[half] = packed
        gram_all[half, pl.ds(me, 1)] = packed[None]
        for dx, dy in far_first:
            @pl.when(has(dx, dy))
            def _():
                gram_copy(half, me, gx + dx, gy + dy).start()

    def shared(half):
        for dev in range(devices):
            @pl.when(me != dev)
            def _():
                gram_copy(half, dev, gx, gy).wait_recv()

        summed = gram_all[half, 0]
        for dev in range(1, devices):
            summed = summed + gram_all[half, dev]
        summed = jnp.where(row < count, summed, 1.0)
        values = {}

        def spread(index):
            return jnp.broadcast_to(summed[:, index : index + 1], (8, nz))

        def gram(i, j):
            if i > j:
                re, im = gram(j, i)
                return re, -im
            if (i, j) not in values:
                re = spread(i * size + j)
                values[i, j] = (re, spread(j * size + i) if i < j else jnp.zeros_like(re))
            return values[i, j]

        return gram

    for r in range(ROUNDS):
        last = r == ROUNDS - 1

        def advance(o, carry):
            wait_halo(r, o)
            if last:
                last_stage(r, o)
                products(2 * r, o)
            else:
                first_stage(r, o)
                second_stage(r, o)
                send_halo(r + 1, o)
            return carry

        lax.fori_loop(0, count, advance, 0)
        if last:
            share(1)
        else:
            def gather(o, carry):
                products(2 * r, o)
                products(2 * r + 1, o)
                return carry

            lax.fori_loop(0, count, gather, 0)
            if r == ROUNDS - 2:
                share(0)

    change, halved, doubled, cross, norm = recurrence(shared(0))
    change = [(a / NEAR, b / NEAR) for a, b in change]

    def combine(o, x, span, coefs):
        total = None
        for j, c in enumerate(coefs):
            term = times_complex(c, (basis[j, 0, o, x, span, :], basis[j, 1, o, x, span, :]))
            total = plus(total, term)
        return total

    for o in range(count):
        def own(values):
            return [
                tuple(jnp.broadcast_to(part[o : o + 1], (8, nz)) for part in value)
                for value in values
            ]

        moves, halves, seconds = (own(change), own(halved), own(doubled))

        def blend(x, carry):
            for y in range(0, by, 8):
                span = slice(LEAD + y, LEAD + y + 8)
                out = slice(y, y + 8)
                for ref, total in (
                    (residual_ref, combine(o, x, span, halves)),
                    (second_ref, combine(o, x, span, seconds)),
                ):
                    ref[0, o, x, out, :] = total[0]
                    ref[1, o, x, out, :] = total[1]
                hat = hats(x, y, residual_ref[0, o, x, out, :], residual_ref[1, o, x, out, :])
                hat_ref[0, o, x, out, :] = hat[0]
                hat_ref[1, o, x, out, :] = hat[1]
                hat = hats(x, y, *combine(o, x, span, moves))
                evolved_ref[0, o, x, out, :] = fields[0, 0, o, x + HALO, span, :] + hat[0]
                evolved_ref[1, o, x, out, :] = fields[0, 1, o, x + HALO, span, :] + hat[1]
            return carry

        sweep(bx, blend, 0)

    for k in range(len(SIDES)):
        @pl.when(has(*SIDES[k]))
        def _():
            if straight(k):
                pot_copy(k).wait_send()
            for r in range(ROUNDS):
                if k in ways(r):
                    for o in range(count):
                        halo_copy(r, o, k).wait_send()

    gram = shared(1)
    column = [gram(i, POWERS) for i in range(size)]
    omega = closing(column, halved, doubled, cross, norm)
    scaled = (omega[0] / NEAR, omega[1] / NEAR)

    for o in range(count):
        step_r, step_e = (
            tuple(jnp.broadcast_to(part[o : o + 1], (8, nz)) for part in value)
            for value in (omega, scaled)
        )

        def finish(x, carry):
            for y in range(0, by, 8):
                out = slice(y, y + 8)
                for ref, other, coef, sign in (
                    (residual_ref, second_ref, step_r, -1.0),
                    (evolved_ref, hat_ref, step_e, 1.0),
                ):
                    term = times_complex(coef, (other[0, o, x, out, :], other[1, o, x, out, :]))
                    ref[0, o, x, out, :] = ref[0, o, x, out, :] + sign * term[0]
                    ref[1, o, x, out, :] = ref[1, o, x, out, :] + sign * term[1]
            return carry

        sweep(bx, finish, 0)

    for half in range(2):
        for dev in range(devices):
            @pl.when(me != dev)
            def _():
                gram_copy(half, me, dev // size_y, dev % size_y).wait_send()


def store_kernel(count, *refs):
    sources, targets, sems = (refs[:count], refs[count : 2 * count], refs[-1])
    copies = [
        pltpu.make_async_copy(sources[k], targets[k], sems.at[k]) for k in range(count)
    ]
    for copy in copies:
        copy.start()
    for copy in copies:
        copy.wait()


def store(arrays):
    count = len(arrays)
    return pl.pallas_call(
        functools.partial(store_kernel, count),
        out_shape=tuple(jax.ShapeDtypeStruct(a.shape, a.dtype) for a in arrays),
        in_specs=[pl.BlockSpec(memory_space=pltpu.VMEM)] * count,
        out_specs=(pl.BlockSpec(memory_space=pltpu.HBM),) * count,
        scratch_shapes=[pltpu.SemaphoreType.DMA((count,))],
        compiler_params=pltpu.CompilerParams(vmem_limit_bytes=1 << 20),
    )(*arrays)


def powers(sizes, orbitals, potential):
    size_x, size_y = sizes
    _, count, bx, by, nz = orbitals.shape
    tall = by + 2 * LEAD
    devices = size_x * size_y
    dma = pltpu.SemaphoreType.DMA
    shape = jax.ShapeDtypeStruct(orbitals.shape, jnp.float32)

    def vmem(*dims):
        return pltpu.VMEM(dims, jnp.float32)

    orbitals, potential = (
        pltpu.with_memory_space_constraint(a, pltpu.HBM) for a in (orbitals, potential)
    )
    results = pl.pallas_call(
        functools.partial(solve_kernel, sizes),
        out_shape=(shape, shape),
        in_specs=[pl.BlockSpec(memory_space=pltpu.HBM)] * 2,
        out_specs=(pl.BlockSpec(memory_space=pltpu.VMEM),) * 2,
        scratch_shapes=[
            vmem(ROUNDS, 2, count, bx + 2 * HALO, tall, nz),
            vmem(2, bx + 4, tall, nz),
            vmem(POWERS + 1, 2, count, bx, tall, nz),
            vmem(bx + 4, tall, nz),
            vmem(bx + 4, tall, nz),
            vmem(bx + 4, tall, nz),
            vmem(bx + 4, tall, nz),
            vmem(*orbitals.shape),
            vmem(*orbitals.shape),
            vmem(2, count, 8, nz),
            vmem(2, 8, nz),
            vmem(2, devices, 8, nz),
            dma((ROUNDS, count, len(SIDES))),
            dma((ROUNDS, count, len(SIDES))),
            dma((len(SIDES),)),
            dma((len(SIDES),)),
            dma((2, devices)),
            dma((2, devices)),
            dma((count + 1,)),
        ],
        compiler_params=pltpu.CompilerParams(
            collective_id=0, has_side_effects=True, vmem_limit_bytes=VMEM_LIMIT
        ),
    )(orbitals, potential)
    return store(results)


def step(sizes, orbitals, potential):
    _, count, bx, by, nz = orbitals.shape
    near = max(sizes) <= ROUNDS
    fits = (POWERS + 2 * ROUNDS) * count * (bx + 8) * (by + 16) * nz <= 1 << 23
    packs = count <= 8 and (POWERS + 1) ** 2 <= nz
    if near and fits and packs and by % 8 == 0 and nz == 128 and bx >= 4:
        return powers(sizes, orbitals, potential)
    return shards(orbitals, potential)


def solution(mesh):
    sizes = (mesh.shape["gx"], mesh.shape["gyz"])
    return jax.shard_map(
        functools.partial(step, sizes),
        mesh=mesh,
        in_specs=(P(None, "orb", "gx", "gyz", None), P("gx", "gyz", None)),
        out_specs=(P(None, "orb", "gx", "gyz", None), P(None, "orb", "gx", "gyz", None)),
        check_vma=False,
    )
```
